32 devices in a mesh: group: 2 (over y), blk: 4 (over z), uly: 4 (over x, core).
Axes of the slice: x: 2, y: 2, z: 4, core: 2. Of those that a mesh axis runs over, the one named last changes fastest.
Arguments:
- query: bfloat16 [768, 3072], P(('group', 'blk', 'uly')), parts along dimension 0, may hold values from -16 to 16
- keys: bfloat16 [768, 3072], P(('group', 'blk', 'uly')), parts along dimension 0, may hold values from -16 to 16
- values: bfloat16 [768, 3072], P(('group', 'blk', 'uly')), parts along dimension 0, may hold values from -6 to 6
- out_weight: bfloat16 [3072, 3072], P('uly', 'blk'), may hold values from -1 to 1
- out_gain: float32 [3072], replicated, may hold values from 0.1 to 1.9
Outputs:
- gated_out: bfloat16 [768, 3072], P(('group', 'blk', 'uly')), parts along dimension 0
The draws below stay inside these ranges and needn't reach their ends.
There are 2 independent parts, one for each index of `group`. The reference program is written for one: setup_inputs(seed, part) draws one part's arguments, and reference() takes and returns one part's arrays. A program takes and returns all parts, laid end to end along the dimension named above; an argument that names none is the same for every part. Nothing has to cross between parts.
All inputs are finite; a program needn't handle non-finite values.
Results may differ from the reference program's by a relative error of at most 0.015.
Values may be sent and summed in bfloat16 or wider, within the bound.
A program may use at most 128 MiB of HBM per device.

```python
import math
import jax
import jax.numpy as jnp
from jax import lax

D = 3072
H = 48
HEAD = 64
TOKENS = 384


def pair_draw(key):
    key_query, key_keys = jax.random.split(jax.random.fold_in(key, 7013), 2)
    query = jnp.clip(1.4 * jax.random.normal(key_query, (TOKENS, D), jnp.float32), -8.0, 8.0)
    keys = jnp.clip(1.4 * jax.random.normal(key_keys, (TOKENS, D), jnp.float32), -8.0, 8.0)
    return (query, keys)


def draw_query(key, part):
    return pair_draw(key)[0].astype(jnp.bfloat16)


def draw_keys(key, part):
    return pair_draw(key)[1].astype(jnp.bfloat16)


def level_of(rng, shape, pieces, smallest, high):
    gain, own = 1.0, jax.random.fold_in(rng, 6)
    for axis_at, shards_of in pieces:
        heights = jnp.exp(jax.random.uniform(jax.random.fold_in(own, axis_at), (shards_of,), jnp.float32, smallest / len(pieces), high / len(pieces)))
        gain = gain * jnp.repeat(heights, shape[axis_at] // shards_of).reshape([-1 if axis == axis_at else 1 for axis in range(len(shape))])
    return gain


def scatter_about(key, shape, deviation, bound, cuts=(), held_as=jnp.bfloat16):
    drawn = jax.random.normal(key, shape, jnp.float32) * deviation
    if len(cuts) > 0:
        drawn = level_of(key, shape, cuts, -0.22, 0.18) * drawn
    return jnp.clip(drawn, min=-bound, max=bound).astype(held_as)


def setup_inputs(seed: int = 0, part: int = 0) -> dict:
    arg_keys = jax.random.split(jax.random.key(seed), 6)
    own_keys = jax.random.split(jax.random.fold_in(arg_keys[5], part), 6)
    query = draw_query(jax.random.fold_in(jax.random.fold_in(arg_keys[5], part), 71), part)
    keys = draw_keys(jax.random.fold_in(jax.random.fold_in(arg_keys[5], part), 71), part)
    values = scatter_about(own_keys[2], (TOKENS, D), 1.0, 6.0, ((0, 16),))
    out_weight = scatter_about(arg_keys[3], (D, D), (HEAD // 2) ** -0.5, 1.0, ((0, 4), (1, 4)))
    out_gain = jnp.clip(1.0 + 0.18 * jax.random.normal(arg_keys[4], (D,), jnp.float32), 0.1, 1.9)
    return {"query": query, "keys": keys, "values": values, "out_weight": out_weight, "out_gain": out_gain}


def reference(query, keys, values, out_weight, out_gain):
    score_scale = 1.0 / math.sqrt(HEAD)
    query_heads = query.reshape(TOKENS, H, HEAD).transpose(1, 0, 2)
    key_heads = keys.reshape(TOKENS, H, HEAD).transpose(1, 0, 2)
    value_heads = values.reshape(TOKENS, H, HEAD).transpose(1, 0, 2)

    def attend(triple):
        query_one, key_one, value_one = triple
        scores = jnp.dot(query_one, key_one.T, preferred_element_type=jnp.float32) * score_scale
        row_max = lax.optimization_barrier(jnp.max(scores, axis=1, keepdims=True))
        weights = jnp.exp(scores - row_max)
        denominator = lax.optimization_barrier(jnp.sum(weights, axis=1, keepdims=True))
        return jnp.dot(weights.astype(jnp.bfloat16), value_one, preferred_element_type=jnp.float32) / denominator
    per_head = lax.map(attend, (query_heads, key_heads, value_heads))
    attended = per_head.transpose(1, 0, 2).reshape(TOKENS, D).astype(jnp.bfloat16)
    projected = jnp.dot(attended, out_weight, preferred_element_type=jnp.float32)
    return (out_gain * projected).astype(jnp.bfloat16)
```

```python
import functools
import math

import jax
import jax.numpy as jnp
from jax import lax
from jax.experimental import pallas as pl
from jax.experimental.pallas import tpu as pltpu
from jax.sharding import PartitionSpec as P

HEAD = 64
LANES = 128
MESH = pl.DeviceIdType.MESH

def make_fold(query_heads, state_now, pieces):
    score_scale = 1.0 / math.sqrt(HEAD)
    head_count = query_heads.shape[1]
    running_max, denominator, weighted = state_now
    key_part, value_part = pieces
    key_count = key_part.shape[0]
    key_heads = key_part.reshape(key_count, head_count, HEAD)
    value_heads = value_part.reshape(key_count, head_count, HEAD)
    scores = (
        jnp.einsum("qhd,khd->qhk", query_heads, key_heads, preferred_element_type=jnp.float32)
        * score_scale
    )
    new_max = jnp.max(scores, axis=2)
    weights = jnp.exp(scores - new_max[:, :, None])
    shrink = jnp.exp(running_max - new_max)
    denominator = denominator * shrink + jnp.sum(weights, axis=2)
    weighted = weighted * shrink[:, :, None] + jnp.einsum(
        "qhk,khd->qhd",
        weights.astype(jnp.bfloat16),
        value_heads,
        preferred_element_type=jnp.float32,
    )
    return (new_max, denominator, weighted)


def initial_state(row_count, head_count):
    return (
        jnp.full((row_count, head_count), -jnp.inf, jnp.float32),
        jnp.zeros((row_count, head_count), jnp.float32),
        jnp.zeros((row_count, head_count, HEAD), jnp.float32),
    )


def on_device(query, keys, values, out_weight, out_gain):
    grouped_q, grouped_k, grouped_v = (
        lax.all_to_all(query, "uly", split_axis=1, concat_axis=0, tiled=True),
        lax.all_to_all(keys, "uly", split_axis=1, concat_axis=0, tiled=True),
        lax.all_to_all(values, "uly", split_axis=1, concat_axis=0, tiled=True),
    )
    row_count = grouped_q.shape[0]
    features = grouped_q.shape[1]
    local_heads = features // HEAD
    query_heads = grouped_q.reshape(row_count, local_heads, HEAD)
    half_heads = local_heads // 2
    half_width = half_heads * HEAD
    low_state = make_fold(
        query_heads[:, :half_heads],
        initial_state(row_count, half_heads),
        (
            lax.all_gather(grouped_k[:, :half_width], "blk", axis=0, tiled=True),
            lax.all_gather(grouped_v[:, :half_width], "blk", axis=0, tiled=True),
        ),
    )
    high_state = make_fold(
        query_heads[:, half_heads:],
        initial_state(row_count, local_heads - half_heads),
        (
            lax.all_gather(grouped_k[:, half_width:], "blk", axis=0, tiled=True),
            lax.all_gather(grouped_v[:, half_width:], "blk", axis=0, tiled=True),
        ),
    )
    denominator = jnp.concatenate([low_state[1], high_state[1]], axis=1)
    weighted = jnp.concatenate([low_state[2], high_state[2]], axis=1)
    attended = (
        (weighted / denominator[:, :, None]).reshape(row_count, features).astype(jnp.bfloat16)
    )
    partial_value = jnp.dot(
        attended,
        lax.all_gather(out_weight, "blk", axis=1, tiled=True),
        preferred_element_type=jnp.float32,
    )
    summed = lax.psum_scatter(
        partial_value.astype(jnp.bfloat16), "uly", scatter_dimension=0, tiled=True
    ).astype(jnp.float32)
    return (out_gain * summed).astype(jnp.bfloat16)


def attend_kernel(
    nb, nu,
    q_hbm, k_hbm, v_hbm, w_hbm, gain_ref, out_ref,
    q_ref, k_ref, v_ref, stage, got, far, w_ref,
    att, acc, part_f32, part_send, part_got, final_send,
    in_sem, w_sem, send_a, recv_a, send_k, recv_k, up_sem,
    send_b, recv_b, pass_b, send_r, recv_r, send_f, recv_f,
):
    nx = nu // 2
    m = nb * nx
    rows, width = q_ref.shape
    pairs = stage.shape[1]
    last = pairs - 1
    depth = w_hbm.shape[0]
    block = nx * rows
    mine_rows = nb * block
    side = nb // 2
    scale = math.log2(math.e) / math.sqrt(HEAD)
    me_b, me_u = lax.axis_index("blk"), lax.axis_index("uly")
    me_x, me_c = me_u // 2, lax.rem(me_u, 2)
    me = me_b * nx + me_x
    my_side = me_b // side
    gate_here = (side - 1) + my_side
    gate_there = side - my_side
    is_gate = me_b == gate_here
    far_side = (1 - my_side) * side

    def turn_of(b, e):
        upward = b // side
        return upward * e + (1 - upward) * (nb - 1 - e)

    def there(b, x):
        return dict(device_id={"blk": b, "uly": 2 * x + me_c}, device_id_type=MESH)

    partner = dict(device_id={"blk": me_b, "uly": 2 * me_x + 1 - me_c}, device_id_type=MESH)
    barrier = pltpu.get_barrier_semaphore()

    pl.semaphore_signal(barrier, inc=1, **partner)
    for d in range(1, nx):
        pl.semaphore_signal(barrier, inc=1, **there(me_b, lax.rem(me_x + d, nx)))
    for b in range(1, nb):

        @pl.when(b > me_b)
        def _():
            for x in range(nx):
                pl.semaphore_signal(barrier, inc=1, **there(b, x))

    loads = [
        pltpu.make_async_copy(src, dst, in_sem.at[i])
        for i, (src, dst) in enumerate(
            ((q_hbm, q_ref), (k_hbm, k_ref), (v_hbm, v_ref),
             (w_hbm, w_ref.at[pl.ds(pl.multiple_of(me_c * depth, depth), depth)])))
    ]
    for load in loads[:3]:
        load.start()
    for load in loads[:3]:
        load.wait()
    loads[3].start()

    for b in range(nb):
        for x in range(nx):
            for p in range(pairs):
                at = ((x * nb + b) * pairs + p) * LANES
                for s, ref in enumerate((q_ref, k_ref, v_ref)):
                    stage[b * nx + x, p, s] = ref[:, pl.ds(at, LANES)]
    for p in range(pairs):
        for s in range(3):
            got[p, s, me] = stage[me, p, s]

    pl.semaphore_wait(barrier, me_b * nx + nx)
    for b in range(nb - 1):

        @pl.when(b < me_b)
        def _():
            for x in range(nx):
                pl.semaphore_signal(up_sem.at[me_b], inc=1, **there(b, x))

    def ship(p, b, x):
        return pltpu.make_async_remote_copy(
            src_ref=stage.at[b * nx + x, p], dst_ref=got.at[p, :, me],
            send_sem=send_a.at[p, b * nx + x], recv_sem=recv_a.at[p, me], **there(b, x))

    def shipped(p, j):
        return pltpu.make_async_remote_copy(
            src_ref=stage.at[j, p], dst_ref=got.at[p, :, j],
            send_sem=send_a.at[p, j], recv_sem=recv_a.at[p, j], **there(me_b, me_x))

    def ship_level(p, b):
        for d in range(nx - 1, -1, -1):
            ship(p, b, lax.rem(me_x + d, nx)).start()

    for p in range(pairs):
        for b in range(nb - 1):

            @pl.when(b < me_b)
            def _():
                ship_level(p, b)
        for d in range(1, nx):
            ship(p, me_b, lax.rem(me_x + d, nx)).start()

    w_swap = pltpu.make_async_remote_copy(
        src_ref=w_hbm, dst_ref=w_ref.at[pl.ds(pl.multiple_of(me_c * depth, depth), depth)],
        send_sem=w_sem.at[0], recv_sem=w_sem.at[1], **partner)
    w_swap.start()

    for b in range(1, nb):

        @pl.when(b > me_b)
        def _():
            pl.semaphore_wait(up_sem.at[b], nx)
            for p in range(last):
                ship_level(p, b)
    for b in range(nb - 1, 0, -1):

        @pl.when(b > me_b)
        def _():
            ship_level(last, b)

    def swap(p):
        return pltpu.make_async_remote_copy(
            src_ref=got.at[p, pl.ds(1, 2)], dst_ref=far.at[p],
            send_sem=send_k.at[p], recv_sem=recv_k.at[p], **partner)

    def against(a, b):
        return lax.dot_general(a, b, (((1,), (1,)), ((), ())), preferred_element_type=jnp.float32)

    low = lax.broadcasted_iota(jnp.int32, (mine_rows, LANES), 1) < HEAD

    def target(d):
        return gate_there if d == 0 else my_side * side + lax.rem(me_b + d, side)

    def piece(ref, p, b, t):
        return ref.at[p, b] if p < last else ref.at[p, b, t]

    def spread(p, d, e):
        t = turn_of(target(d), e)
        slot = t if p == last else 0
        return pltpu.make_async_remote_copy(
            src_ref=piece(att, p, me_b, t), dst_ref=piece(att, p, me_b, t),
            send_sem=send_b.at[p, d, slot], recv_sem=recv_b.at[p, me_b, slot],
            **there(target(d), me_x))

    def spread_in(p, b, t):
        slot = t if p == last else 0
        return pltpu.make_async_remote_copy(
            src_ref=piece(att, p, b, t), dst_ref=piece(att, p, b, t),
            send_sem=send_b.at[p, 0, slot], recv_sem=recv_b.at[p, b, slot], **there(me_b, me_x))

    def pass_on(p, d, b, t):
        slot = t if p == last else 0
        return pltpu.make_async_remote_copy(
            src_ref=piece(att, p, b, t), dst_ref=piece(att, p, b, t),
            send_sem=pass_b.at[p, d, b, slot], recv_sem=recv_b.at[p, b, slot],
            **there(target(d), me_x))

    def parts_of(p):
        return range(nb) if p == last else range(1)

    for p in range(pairs):

        @pl.loop(1, m)
        def _(d):
            shipped(p, lax.rem(me + m - d, m)).wait_recv()

        swap(p).start()
        q_all = jnp.concatenate([got[p, 0, i].astype(jnp.float32) for i in range(m)], axis=0)
        q_two = jnp.concatenate(
            [jnp.where(low, q_all, 0.0), jnp.where(low, 0.0, q_all)], axis=0).astype(jnp.bfloat16)
        swap(p).wait_recv()
        k_all, v_all = (
            jnp.concatenate(
                [got[p, s, i].astype(jnp.float32) for i in range(m)]
                + [far[p, s - 1, i].astype(jnp.float32) for i in range(m)], axis=0
            ).astype(jnp.bfloat16)
            for s in (1, 2))
        scores = against(q_two, k_all)
        top = jnp.max(scores, axis=1, keepdims=True)
        weights = jnp.exp2((scores - top) * scale)
        total = jnp.sum(weights, axis=1, keepdims=True)
        both = jnp.dot(
            weights.astype(jnp.bfloat16), v_all, preferred_element_type=jnp.float32) / total
        joined = jnp.where(low, both[:mine_rows], both[mine_rows:]).astype(jnp.bfloat16)
        for t in range(nb):
            att[p, me_b, t] = joined[t * block:(t + 1) * block]
        for e in parts_of(p):
            for d in range(side):
                spread(p, d, e).start()

    def forward(p, t):
        for i in range(side):
            b = far_side + i
            spread_in(p, b, t).wait_recv()

            @pl.when(is_gate)
            def _():
                for d in range(1, side):
                    pass_on(p, d, b, t).start()

    def settle(p, t):
        forward(p, t)
        for d in range(1, side):
            spread_in(p, target(d), t).wait_recv()

    def weight_of(p):
        return jnp.concatenate(
            [w_ref[pl.ds((b * pairs + p) * LANES, LANES)] for b in range(nb)], axis=0)

    loads[3].wait()
    w_swap.wait_recv()
    for p in range(last):
        settle(p, 0)
        seen = jnp.concatenate(
            [att[p, b].reshape(mine_rows, LANES) for b in range(nb)], axis=1)
        part = jnp.dot(seen, weight_of(p), preferred_element_type=jnp.float32)
        part = part.reshape(acc.shape)
        if p == 0:
            acc[...] = part
        else:
            acc[...] += part

    def scatter(t, d):
        x = lax.rem(me_x + d, nx)
        return pltpu.make_async_remote_copy(
            src_ref=part_send.at[t, x], dst_ref=part_got.at[t, me_x],
            send_sem=send_r.at[t, d], recv_sem=recv_r.at[t, me_x], **there(me_b, x))

    def scatter_in(t, d):
        x = lax.rem(me_x + nx - d, nx)
        return pltpu.make_async_remote_copy(
            src_ref=part_send.at[t, x], dst_ref=part_got.at[t, x],
            send_sem=send_r.at[t, d], recv_sem=recv_r.at[t, x], **there(me_b, me_x))

    def final(t):
        return pltpu.make_async_remote_copy(
            src_ref=final_send.at[t], dst_ref=out_ref.at[me_b],
            send_sem=send_f.at[t], recv_sem=recv_f.at[me_b], **there(t, me_x))

    def final_in(d):
        b = lax.rem(me_b + nb - d, nb)
        return pltpu.make_async_remote_copy(
            src_ref=final_send.at[b], dst_ref=out_ref.at[b],
            send_sem=send_f.at[b], recv_sem=recv_f.at[b], **there(me_b, me_x))

    def reduce(e):
        t = turn_of(me_b, e)
        total = part_f32[t, me_x]
        for d in range(1, nx):
            scatter_in(t, d).wait_recv()
            total += part_got[t, lax.rem(me_x + nx - d, nx)].astype(jnp.float32)
        gated = (gain_ref[me_b] * total).astype(jnp.bfloat16)

        @pl.when(me_b == t)
        def _():
            out_ref[t] = gated

        @pl.when(me_b != t)
        def _():
            final_send[t] = gated
            final(t).start()

    lag = 2
    for e in range(nb):
        t = turn_of(me_b, e)
        settle(last, t)
        seen = jnp.concatenate([att[last, b, t] for b in range(nb)], axis=1)
        part = jnp.dot(seen, weight_of(last), preferred_element_type=jnp.float32)
        if pairs > 1:
            part += acc[t]
        for x in range(nx):
            one = part[x * rows:(x + 1) * rows]
            part_f32[t, x] = one
            part_send[t, x] = one.astype(jnp.bfloat16)
        for d in range(1, nx):
            scatter(t, d).start()
        if e >= lag:
            reduce(e - lag)
    for e in range(nb - lag, nb):
        reduce(e)

    for d in range(1, nb):
        final_in(d).wait_recv()

    w_swap.wait_send()
    for p in range(pairs):
        swap(p).wait_send()

        @pl.loop(1, m)
        def _(d):
            shipped(p, lax.rem(me + d, m)).wait_send()

        for e in parts_of(p):
            for d in range(side):
                spread(p, d, e).wait_send()

            @pl.when(is_gate)
            def _():
                for i in range(side):
                    for d in range(1, side):
                        pass_on(p, d, far_side + i, e).wait_send()
    for t in range(nb):
        for d in range(1, nx):
            scatter(t, d).wait_send()

        @pl.when(me_b != t)
        def _():
            final(t).wait_send()


def fused(nb, nu, query, keys, values, out_weight, out_gain):
    nx = nu // 2
    m = nb * nx
    rows, width = query.shape
    pairs = width // LANES // m
    depth, columns = out_weight.shape
    bf16, f32 = jnp.bfloat16, jnp.float32
    vmem, dma = pltpu.VMEM, pltpu.SemaphoreType.DMA
    in_vmem = pl.BlockSpec(memory_space=pltpu.VMEM)
    in_place = pl.BlockSpec(memory_space=pl.ANY)
    block, side = nx * rows, nb // 2
    gathered = pl.pallas_call(
        functools.partial(attend_kernel, nb, nu),
        out_shape=jax.ShapeDtypeStruct((nb, rows, columns), bf16),
        in_specs=[in_place, in_place, in_place, in_place, in_vmem],
        out_specs=in_vmem,
        scratch_shapes=[
            vmem((rows, width), bf16), vmem((rows, width), bf16), vmem((rows, width), bf16),
            vmem((m, pairs, 3, rows, LANES), bf16),
            vmem((pairs, 3, m, rows, LANES), bf16),
            vmem((pairs, 2, m, rows, LANES), bf16),
            vmem((2 * depth, columns), bf16),
            vmem((pairs, nb, nb, block, LANES), bf16),
            vmem((nb, block, columns), f32),
            vmem((nb, nx, rows, columns), f32),
            vmem((nb, nx, rows, columns), bf16),
            vmem((nb, nx, rows, columns), bf16),
            vmem((nb, rows, columns), bf16),
            dma((4,)), dma((2,)), dma((pairs, m)), dma((pairs, m)), dma((pairs,)), dma((pairs,)),
            pltpu.SemaphoreType.REGULAR((nb,)),
            dma((pairs, side, nb)), dma((pairs, nb, nb)), dma((pairs, side, nb, nb)),
            dma((nb, nx)), dma((nb, nx)), dma((nb,)), dma((nb,)),
        ],
        compiler_params=pltpu.CompilerParams(collective_id=0, has_side_effects=True),
    )(query, keys, values, out_weight, out_gain.reshape(nb, 1, columns))
    return gathered.transpose(1, 0, 2).reshape(rows, width)


def on_any(nb, nu, query, keys, values, out_weight, out_gain):
    rows, width = query.shape
    suits = (
        nu % 2 == 0 and nb % 2 == 0 and width % (LANES * nb * nu // 2) == 0
        and rows % 8 == 0 and (nu // 2 * rows) % 16 == 0 and (width // nb) % LANES == 0
    )
    plan = functools.partial(fused, nb, nu) if suits else on_device
    return plan(query, keys, values, out_weight, out_gain)


def solution(mesh):
    in_specs = (
        P(("group", "blk", "uly"), None),
        P(("group", "blk", "uly"), None),
        P(("group", "blk", "uly"), None),
        P("uly", "blk"),
        P(),
    )
    out_specs = P(("group", "blk", "uly"), None)
    body = functools.partial(on_any, mesh.shape["blk"], mesh.shape["uly"])
    return jax.shard_map(
        body, mesh=mesh, in_specs=in_specs, out_specs=out_specs, check_vma=False
    )
```

```python
import functools
import math

import jax
import jax.numpy as jnp
from jax import lax
from jax.experimental import pallas as pl
from jax.experimental.pallas import tpu as pltpu
from jax.sharding import PartitionSpec as P

HEAD = 64
LANES = 128
MESH = pl.DeviceIdType.MESH

def make_fold(query_heads, state_now, pieces):
    score_scale = 1.0 / math.sqrt(HEAD)
    head_count = query_heads.shape[1]
    running_max, denominator, weighted = state_now
    key_part, value_part = pieces
    key_count = key_part.shape[0]
    key_heads = key_part.reshape(key_count, head_count, HEAD)
    value_heads = value_part.reshape(key_count, head_count, HEAD)
    scores = (
        jnp.einsum("qhd,khd->qhk", query_heads, key_heads, preferred_element_type=jnp.float32)
        * score_scale
    )
    new_max = jnp.max(scores, axis=2)
    weights = jnp.exp(scores - new_max[:, :, None])
    shrink = jnp.exp(running_max - new_max)
    denominator = denominator * shrink + jnp.sum(weights, axis=2)
    weighted = weighted * shrink[:, :, None] + jnp.einsum(
        "qhk,khd->qhd",
        weights.astype(jnp.bfloat16),
        value_heads,
        preferred_element_type=jnp.float32,
    )
    return (new_max, denominator, weighted)


def initial_state(row_count, head_count):
    return (
        jnp.full((row_count, head_count), -jnp.inf, jnp.float32),
        jnp.zeros((row_count, head_count), jnp.float32),
        jnp.zeros((row_count, head_count, HEAD), jnp.float32),
    )


def on_device(query, keys, values, out_weight, out_gain):
    grouped_q, grouped_k, grouped_v = (
        lax.all_to_all(query, "uly", split_axis=1, concat_axis=0, tiled=True),
        lax.all_to_all(keys, "uly", split_axis=1, concat_axis=0, tiled=True),
        lax.all_to_all(values, "uly", split_axis=1, concat_axis=0, tiled=True),
    )
    row_count = grouped_q.shape[0]
    features = grouped_q.shape[1]
    local_heads = features // HEAD
    query_heads = grouped_q.reshape(row_count, local_heads, HEAD)
    half_heads = local_heads // 2
    half_width = half_heads * HEAD
    low_state = make_fold(
        query_heads[:, :half_heads],
        initial_state(row_count, half_heads),
        (
            lax.all_gather(grouped_k[:, :half_width], "blk", axis=0, tiled=True),
            lax.all_gather(grouped_v[:, :half_width], "blk", axis=0, tiled=True),
        ),
    )
    high_state = make_fold(
        query_heads[:, half_heads:],
        initial_state(row_count, local_heads - half_heads),
        (
            lax.all_gather(grouped_k[:, half_width:], "blk", axis=0, tiled=True),
            lax.all_gather(grouped_v[:, half_width:], "blk", axis=0, tiled=True),
        ),
    )
    denominator = jnp.concatenate([low_state[1], high_state[1]], axis=1)
    weighted = jnp.concatenate([low_state[2], high_state[2]], axis=1)
    attended = (
        (weighted / denominator[:, :, None]).reshape(row_count, features).astype(jnp.bfloat16)
    )
    partial_value = jnp.dot(
        attended,
        lax.all_gather(out_weight, "blk", axis=1, tiled=True),
        preferred_element_type=jnp.float32,
    )
    summed = lax.psum_scatter(
        partial_value.astype(jnp.bfloat16), "uly", scatter_dimension=0, tiled=True
    ).astype(jnp.float32)
    return (out_gain * summed).astype(jnp.bfloat16)


def attend_kernel(
    nb, nu,
    q_hbm, k_hbm, v_hbm, w_hbm, gain_hbm, out_ref,
    qkv_ref, gain_ref, stage, got, far, w_ref,
    att, acc, part_f32, part_send, part_got, final_send,
    in_sem, w_in, w_sent, w_came, a_sent, a_came, k_sent, k_came, up_sem,
    b_sent, b_came, b_last, passed, r_sent, r_came, f_sent, f_came,
):
    nx = nu // 2
    m = nb * nx
    rows, width = q_hbm.shape
    pairs = stage.shape[1]
    last = pairs - 1
    depth = w_hbm.shape[0]
    block = nx * rows
    mine_rows = nb * block
    side = nb // 2
    scale = math.log2(math.e) / math.sqrt(HEAD)
    me_b, me_u = lax.axis_index("blk"), lax.axis_index("uly")
    me_x, me_c = me_u // 2, lax.rem(me_u, 2)
    me = me_b * nx + me_x
    my_side = me_b // side
    gate_here = (side - 1) + my_side
    gate_there = side - my_side
    is_gate = me_b == gate_here
    far_side = (1 - my_side) * side

    def turn_of(b, e):
        upward = b // side
        return upward * e + (1 - upward) * (nb - 1 - e)

    def there(b, x):
        return dict(device_id={"blk": b, "uly": 2 * x + me_c}, device_id_type=MESH)

    partner = dict(device_id={"blk": me_b, "uly": 2 * me_x + 1 - me_c}, device_id_type=MESH)

    def await_bytes(ref, sem):
        pltpu.make_async_copy(ref, ref, sem).wait()

    def when(condition, action):
        pl.when(condition)(action)

    barrier = pltpu.get_barrier_semaphore()
    pl.semaphore_signal(barrier, inc=1, **partner)
    for d in range(1, nx):
        pl.semaphore_signal(barrier, inc=1, **there(me_b, lax.rem(me_x + d, nx)))
    for b in range(1, nb):

        @pl.when(b > me_b)
        def _():
            for x in range(nx):
                pl.semaphore_signal(barrier, inc=1, **there(b, x))

    for s, ref in enumerate((q_hbm, k_hbm, v_hbm)):
        pltpu.make_async_copy(ref, qkv_ref.at[s], in_sem).start()
    w_mine = w_ref.at[pl.ds(pl.multiple_of(me_c * depth, depth), depth)]
    with jax.named_scope("load"):
        await_bytes(qkv_ref, in_sem)
    w_load = pltpu.make_async_copy(w_hbm, w_mine, w_in)
    gain_load = pltpu.make_async_copy(gain_hbm, gain_ref, in_sem)
    w_load.start()
    gain_load.start()

    for b in range(nb):
        for x in range(nx):
            for p in range(pairs):
                at = ((x * nb + b) * pairs + p) * LANES
                for s in range(3):
                    stage[b * nx + x, p, s] = qkv_ref[s, :, pl.ds(at, LANES)]
    for p in range(pairs):
        for s in range(3):
            got[p, s, me] = stage[me, p, s]

    with jax.named_scope("barrier"):
        pl.semaphore_wait(barrier, me_b * nx + nx)
    for b in range(nb - 1):

        @pl.when(b < me_b)
        def _():
            for x in range(nx):
                pl.semaphore_signal(up_sem.at[me_b - 1], inc=1, **there(b, x))

    def ship(p, b, x):
        pltpu.make_async_remote_copy(
            src_ref=stage.at[b * nx + x, p], dst_ref=got.at[p, :, me],
            send_sem=a_sent, recv_sem=a_came.at[p], **there(b, x)).start()

    def ship_level(p, b):
        for d in range(nx - 1, -1, -1):
            ship(p, b, lax.rem(me_x + d, nx))

    def ship_beside(p):
        for d in range(1, nx):
            ship(p, me_b, lax.rem(me_x + d, nx))

    for p in range(pairs):
        for b in range(nb - 1):
            when(b < me_b, lambda: ship_level(p, b))
        ship_beside(p)

    w_swap = pltpu.make_async_remote_copy(
        src_ref=w_mine, dst_ref=w_mine, send_sem=w_sent, recv_sem=w_came, **partner)
    w_load.wait()
    gain_load.wait()
    w_swap.start()

    for b in range(1, nb):

        @pl.when(b > me_b)
        def _():
            with jax.named_scope(f"up{b}"):
                pl.semaphore_wait(up_sem.at[b - 1], nx)
            for p in range(min(2, pairs)):
                ship_level(p, b)
    for p in range(2, pairs):
        for b in range(nb - 1, 0, -1):
            when(b > me_b, lambda: ship_level(p, b))

    def swap(p):
        return pltpu.make_async_remote_copy(
            src_ref=got.at[p, pl.ds(1, 2)], dst_ref=far.at[p],
            send_sem=k_sent, recv_sem=k_came.at[p], **partner)

    def against(a, b):
        return lax.dot_general(a, b, (((1,), (1,)), ((), ())), preferred_element_type=jnp.float32)

    low = lax.broadcasted_iota(jnp.int32, (mine_rows, LANES), 1) < HEAD

    def target(d):
        return gate_there if d == 0 else my_side * side + lax.rem(me_b + d, side)

    def slot_of(origin, b):
        return origin - (origin > b)

    def spread(p, d, e):
        t = turn_of(target(d), e)
        whole = p < last
        piece = att.at[p, me_b] if whole else att.at[p, me_b, t]
        sem = b_came.at[p, me_b] if whole else b_last.at[me_b, t]
        pltpu.make_async_remote_copy(
            src_ref=piece, dst_ref=piece, send_sem=b_sent, recv_sem=sem,
            **there(target(d), me_x)).start()

    def spread_in(p, b, t):
        if p < last:
            await_bytes(att.at[p, b], b_came.at[p, b])
        else:
            await_bytes(att.at[p, b, t], b_last.at[b, t])

    def pass_on(p, d, b, t):
        whole = p < last
        piece = att.at[p, b] if whole else att.at[p, b, t]
        sem = b_came.at[p, b] if whole else b_last.at[b, t]
        pltpu.make_async_remote_copy(
            src_ref=piece, dst_ref=piece, send_sem=passed, recv_sem=sem,
            **there(target(d), me_x)).start()

    def spread_all(p):
        for e in range(nb if p == last else 1):
            for d in range(side):
                spread(p, d, e)

    def forward(p, t):
        for i in range(side):
            b = far_side + my_side * i + (1 - my_side) * (side - 1 - i)
            spread_in(p, b, t)

            @pl.when(is_gate)
            def _():
                for d in range(1, side):
                    pass_on(p, d, b, t)

    for p in range(pairs):
        with jax.named_scope(f"wA{p}"):
            await_bytes(got.at[p, :, pl.ds(0, m - 1)], a_came.at[p])
        swap(p).start()
        if p == last:
            for early in range(last):
                when(jnp.logical_not(is_gate), lambda: spread_all(early))
        q_all = jnp.concatenate([got[p, 0, i].astype(jnp.float32) for i in range(m)], axis=0)
        q_two = jnp.concatenate(
            [jnp.where(low, q_all, 0.0), jnp.where(low, 0.0, q_all)], axis=0).astype(jnp.bfloat16)
        with jax.named_scope(f"wK{p}"):
            await_bytes(far.at[p], k_came.at[p])
        k_all, v_all = (
            jnp.concatenate(
                [got[p, s, i].astype(jnp.float32) for i in range(m)]
                + [far[p, s - 1, i].astype(jnp.float32) for i in range(m)], axis=0
            ).astype(jnp.bfloat16)
            for s in (1, 2))
        scores = against(q_two, k_all)
        top = jnp.max(scores, axis=1, keepdims=True)
        weights = jnp.exp2((scores - top) * scale)
        total = jnp.sum(weights, axis=1, keepdims=True)
        both = jnp.dot(
            weights.astype(jnp.bfloat16), v_all, preferred_element_type=jnp.float32) / total
        joined = jnp.where(low, both[:mine_rows], both[mine_rows:]).astype(jnp.bfloat16)
        for t in range(nb):
            att[p, me_b, t] = joined[t * block:(t + 1) * block]
        with jax.named_scope(f"sB{p}"):
            if p == last:
                spread_all(p)
            else:
                when(is_gate, lambda: spread_all(p))

    def settle(p, t):
        forward(p, t)
        for d in range(1, side):
            spread_in(p, target(d), t)

    def weight_of(p):
        return jnp.concatenate(
            [w_ref[pl.ds((b * pairs + p) * LANES, LANES)] for b in range(nb)], axis=0)

    with jax.named_scope("wW"):
        await_bytes(w_mine, w_came)
    for p in range(last):
        with jax.named_scope(f"wB{p}"):
            settle(p, 0)
        seen = jnp.concatenate(
            [att[p, b].reshape(mine_rows, LANES) for b in range(nb)], axis=1)
        part = jnp.dot(seen, weight_of(p), preferred_element_type=jnp.float32).reshape(acc.shape)
        if p == 0:
            acc[...] = part
        else:
            acc[...] += part

    def scatter(t, d):
        x = lax.rem(me_x + d, nx)
        pltpu.make_async_remote_copy(
            src_ref=part_send.at[t, x], dst_ref=part_got.at[t, me_x],
            send_sem=r_sent, recv_sem=r_came.at[t, d - 1], **there(me_b, x)).start()

    def reduce(e):
        t = turn_of(me_b, e)
        total = part_f32[t, me_x]
        for d in range(1, nx):
            x = lax.rem(me_x + nx - d, nx)
            with jax.named_scope(f"wR{e}"):
                await_bytes(part_got.at[t, x], r_came.at[t, d - 1])
            total += part_got[t, x].astype(jnp.float32)
        gated = (gain_ref[me_b] * total).astype(jnp.bfloat16)

        @pl.when(me_b == t)
        def _():
            out_ref[t] = gated

        @pl.when(me_b != t)
        def _():
            final_send[t] = gated
            pltpu.make_async_remote_copy(
                src_ref=final_send.at[t], dst_ref=out_ref.at[me_b],
                send_sem=f_sent, recv_sem=f_came, **there(t, me_x)).start()

    for e in range(nb):
        t = turn_of(me_b, e)
        with jax.named_scope(f"wBl{e}"):
            settle(last, t)
        seen = jnp.concatenate([att[last, b, t] for b in range(nb)], axis=1)
        part = jnp.dot(seen, weight_of(last), preferred_element_type=jnp.float32)
        if pairs > 1:
            part += acc[t]
        for x in range(nx):
            one = part[x * rows:(x + 1) * rows]
            part_f32[t, x] = one
            part_send[t, x] = one.astype(jnp.bfloat16)
        for d in range(1, nx):
            scatter(t, d)
        if e >= 2:
            reduce(e - 2)
    for e in range(nb - 2, nb):
        reduce(e)

    with jax.named_scope("wF"):
        await_bytes(out_ref.at[pl.ds(0, nb - 1)], f_came)

    with jax.named_scope("drain"):
        w_swap.wait_send()
        await_bytes(stage.at[pl.ds(0, m - 1)], a_sent)
        await_bytes(far, k_sent)
        await_bytes(att.at[:, pl.ds(0, side)], b_sent)

        @pl.when(is_gate)
        def _():
            await_bytes(att.at[:, pl.ds(0, side * (side - 1))], passed)

        await_bytes(part_send.at[:, pl.ds(0, nx - 1)], r_sent)
        await_bytes(final_send.at[pl.ds(0, nb - 1)], f_sent)


def fused(nb, nu, query, keys, values, out_weight, out_gain):
    nx = nu // 2
    m = nb * nx
    rows, width = query.shape
    pairs = width // LANES // m
    depth, columns = out_weight.shape
    bf16, f32 = jnp.bfloat16, jnp.float32
    vmem, dma = pltpu.VMEM, pltpu.SemaphoreType.DMA
    in_hbm = pl.BlockSpec(memory_space=pltpu.HBM)
    block = nx * rows
    gathered = pl.pallas_call(
        functools.partial(attend_kernel, nb, nu),
        out_shape=vmem((nb, rows, columns), bf16),
        in_specs=[in_hbm] * 5,
        out_specs=pl.BlockSpec(memory_space=pltpu.VMEM),
        scratch_shapes=[
            vmem((3, rows, width), bf16),
            vmem((nb, 1, columns), f32),
            vmem((m, pairs, 3, rows, LANES), bf16),
            vmem((pairs, 3, m, rows, LANES), bf16),
            vmem((pairs, 2, m, rows, LANES), bf16),
            vmem((2 * depth, columns), bf16),
            vmem((pairs, nb, nb, block, LANES), bf16),
            vmem((nb, block, columns), f32),
            vmem((nb, nx, rows, columns), f32),
            vmem((nb, nx, rows, columns), bf16),
            vmem((nb, nx, rows, columns), bf16),
            vmem((nb, rows, columns), bf16),
            dma, dma, dma, dma, dma, dma((pairs,)), dma, dma((pairs,)),
            pltpu.SemaphoreType.REGULAR((nb - 1,)),
            dma, dma((pairs, nb)), dma((nb, nb)), dma, dma, dma((nb, nx - 1)), dma, dma,
        ],
        compiler_params=pltpu.CompilerParams(
            collective_id=0, has_side_effects=True),
    )(query, keys, values, out_weight, out_gain.reshape(nb, 1, columns))
    return gathered.transpose(1, 0, 2).reshape(rows, width)


def on_any(nb, nu, query, keys, values, out_weight, out_gain):
    rows, width = query.shape
    suits = (
        nu % 2 == 0 and nu > 2 and nb % 2 == 0 and width % (LANES * nb * nu // 2) == 0
        and rows % 8 == 0 and (nu // 2 * rows) % 16 == 0 and (width // nb) % LANES == 0
    )
    plan = functools.partial(fused, nb, nu) if suits else on_device
    return plan(query, keys, values, out_weight, out_gain)


def solution(mesh):
    in_specs = (
        P(("group", "blk", "uly"), None),
        P(("group", "blk", "uly"), None),
        P(("group", "blk", "uly"), None),
        P("uly", "blk"),
        P(),
    )
    out_specs = P(("group", "blk", "uly"), None)
    body = functools.partial(on_any, mesh.shape["blk"], mesh.shape["uly"])
    return jax.shard_map(
        body, mesh=mesh, in_specs=in_specs, out_specs=out_specs, check_vma=False
    )
```

```python
import functools
import math

import jax
import jax.numpy as jnp
from jax import lax
from jax.experimental import pallas as pl
from jax.experimental.pallas import tpu as pltpu
from jax.sharding import PartitionSpec as P

HEAD = 64
LANES = 128
MESH = pl.DeviceIdType.MESH

def make_fold(query_heads, state_now, pieces):
    score_scale = 1.0 / math.sqrt(HEAD)
    head_count = query_heads.shape[1]
    running_max, denominator, weighted = state_now
    key_part, value_part = pieces
    key_count = key_part.shape[0]
    key_heads = key_part.reshape(key_count, head_count, HEAD)
    value_heads = value_part.reshape(key_count, head_count, HEAD)
    scores = (
        jnp.einsum("qhd,khd->qhk", query_heads, key_heads, preferred_element_type=jnp.float32)
        * score_scale
    )
    new_max = jnp.max(scores, axis=2)
    weights = jnp.exp(scores - new_max[:, :, None])
    shrink = jnp.exp(running_max - new_max)
    denominator = denominator * shrink + jnp.sum(weights, axis=2)
    weighted = weighted * shrink[:, :, None] + jnp.einsum(
        "qhk,khd->qhd",
        weights.astype(jnp.bfloat16),
        value_heads,
        preferred_element_type=jnp.float32,
    )
    return (new_max, denominator, weighted)


def initial_state(row_count, head_count):
    return (
        jnp.full((row_count, head_count), -jnp.inf, jnp.float32),
        jnp.zeros((row_count, head_count), jnp.float32),
        jnp.zeros((row_count, head_count, HEAD), jnp.float32),
    )


def on_device(query, keys, values, out_weight, out_gain):
    grouped_q, grouped_k, grouped_v = (
        lax.all_to_all(query, "uly", split_axis=1, concat_axis=0, tiled=True),
        lax.all_to_all(keys, "uly", split_axis=1, concat_axis=0, tiled=True),
        lax.all_to_all(values, "uly", split_axis=1, concat_axis=0, tiled=True),
    )
    row_count = grouped_q.shape[0]
    features = grouped_q.shape[1]
    local_heads = features // HEAD
    query_heads = grouped_q.reshape(row_count, local_heads, HEAD)
    half_heads = local_heads // 2
    half_width = half_heads * HEAD
    low_state = make_fold(
        query_heads[:, :half_heads],
        initial_state(row_count, half_heads),
        (
            lax.all_gather(grouped_k[:, :half_width], "blk", axis=0, tiled=True),
            lax.all_gather(grouped_v[:, :half_width], "blk", axis=0, tiled=True),
        ),
    )
    high_state = make_fold(
        query_heads[:, half_heads:],
        initial_state(row_count, local_heads - half_heads),
        (
            lax.all_gather(grouped_k[:, half_width:], "blk", axis=0, tiled=True),
            lax.all_gather(grouped_v[:, half_width:], "blk", axis=0, tiled=True),
        ),
    )
    denominator = jnp.concatenate([low_state[1], high_state[1]], axis=1)
    weighted = jnp.concatenate([low_state[2], high_state[2]], axis=1)
    attended = (
        (weighted / denominator[:, :, None]).reshape(row_count, features).astype(jnp.bfloat16)
    )
    partial_value = jnp.dot(
        attended,
        lax.all_gather(out_weight, "blk", axis=1, tiled=True),
        preferred_element_type=jnp.float32,
    )
    summed = lax.psum_scatter(
        partial_value.astype(jnp.bfloat16), "uly", scatter_dimension=0, tiled=True
    ).astype(jnp.float32)
    return (out_gain * summed).astype(jnp.bfloat16)


def attend_kernel(
    nb, nu,
    q_hbm, k_hbm, v_hbm, w_hbm, gain_hbm, out_ref,
    qkv_ref, gain_ref, stage, got, far, w_ref,
    att, acc, part_f32, part_send, part_got, final_send,
    in_sem, w_in, w_sent, w_came, a_sent, a_came, k_sent, k_came, up_sem,
    b_sent, b_came, b_last, passed, r_sent, r_came, f_sent, f_came,
):
    nx = nu // 2
    m = nb * nx
    rows, width = q_hbm.shape
    pairs = stage.shape[1]
    last = pairs - 1
    depth = w_hbm.shape[0]
    block = nx * rows
    mine_rows = nb * block
    side = nb // 2
    scale = math.log2(math.e) / math.sqrt(HEAD)
    me_b, me_u = lax.axis_index("blk"), lax.axis_index("uly")
    me_x, me_c = me_u // 2, lax.rem(me_u, 2)
    me = me_b * nx + me_x
    my_side = me_b // side
    gate_here = (side - 1) + my_side
    gate_there = side - my_side
    is_gate = me_b == gate_here
    held = (me_b < side) & jnp.logical_not(is_gate)
    far_side = (1 - my_side) * side

    def turn_of(b, e):
        upward = b // side
        return upward * e + (1 - upward) * (nb - 1 - e)

    def there(b, x):
        return dict(device_id={"blk": b, "uly": 2 * x + me_c}, device_id_type=MESH)

    partner = dict(device_id={"blk": me_b, "uly": 2 * me_x + 1 - me_c}, device_id_type=MESH)

    def await_bytes(ref, sem):
        pltpu.make_async_copy(ref, ref, sem).wait()

    def when(condition, action):
        pl.when(condition)(action)

    barrier = pltpu.get_barrier_semaphore()
    pl.semaphore_signal(barrier, inc=1, **partner)
    for d in range(1, nx):
        pl.semaphore_signal(barrier, inc=1, **there(me_b, lax.rem(me_x + d, nx)))
    for b in range(1, nb):

        @pl.when(b > me_b)
        def _():
            for x in range(nx):
                pl.semaphore_signal(barrier, inc=1, **there(b, x))

    for s, ref in enumerate((q_hbm, k_hbm, v_hbm)):
        pltpu.make_async_copy(ref, qkv_ref.at[s], in_sem).start()
    w_mine = w_ref.at[pl.ds(pl.multiple_of(me_c * depth, depth), depth)]
    with jax.named_scope("barrier"):
        pl.semaphore_wait(barrier, me_b * nx + nx)
    for b in range(nb - 1):

        @pl.when(b < me_b)
        def _():
            for x in range(nx):
                pl.semaphore_signal(up_sem.at[me_b - 1], inc=1, **there(b, x))

    with jax.named_scope("load"):
        await_bytes(qkv_ref, in_sem)
    w_load = pltpu.make_async_copy(w_hbm, w_mine, w_in)
    gain_load = pltpu.make_async_copy(gain_hbm, gain_ref, in_sem)
    w_load.start()
    gain_load.start()

    for b in range(nb):
        for x in range(nx):
            for p in range(pairs):
                at = ((x * nb + b) * pairs + p) * LANES
                for s in range(3):
                    stage[b * nx + x, p, s] = qkv_ref[s, :, pl.ds(at, LANES)]
    for p in range(pairs):
        for s in range(3):
            got[p, s, me] = stage[me, p, s]


    def ship(p, b, x):
        pltpu.make_async_remote_copy(
            src_ref=stage.at[b * nx + x, p], dst_ref=got.at[p, :, me],
            send_sem=a_sent, recv_sem=a_came.at[p], **there(b, x)).start()

    def ship_level(p, b):
        for d in range(nx - 1, -1, -1):
            ship(p, b, lax.rem(me_x + d, nx))

    def ship_beside(p):
        for d in range(1, nx):
            ship(p, me_b, lax.rem(me_x + d, nx))

    for p in range(pairs):
        for b in range(nb - 1):
            when(b < me_b, lambda: ship_level(p, b))
        ship_beside(p)

    w_swap = pltpu.make_async_remote_copy(
        src_ref=w_mine, dst_ref=w_mine, send_sem=w_sent, recv_sem=w_came, **partner)
    w_load.wait()
    gain_load.wait()
    w_swap.start()

    for b in range(1, nb):

        @pl.when(b > me_b)
        def _():
            with jax.named_scope(f"up{b}"):
                pl.semaphore_wait(up_sem.at[b - 1], nx)
            for p in range(min(1, pairs)):
                ship_level(p, b)
    for p in range(1, pairs):
        for b in range(nb - 1, 0, -1):
            when((b > me_b) & (me_b > 0), lambda: ship_level(p, b))

    def swap(p):
        return pltpu.make_async_remote_copy(
            src_ref=got.at[p, pl.ds(1, 2)], dst_ref=far.at[p],
            send_sem=k_sent, recv_sem=k_came.at[p], **partner)

    def against(a, b):
        return lax.dot_general(a, b, (((1,), (1,)), ((), ())), preferred_element_type=jnp.float32)

    low = lax.broadcasted_iota(jnp.int32, (mine_rows, LANES), 1) < HEAD

    def target(d):
        return gate_there if d == 0 else my_side * side + lax.rem(me_b + d, side)

    def slot_of(origin, b):
        return origin - (origin > b)

    def spread(p, d, e):
        t = turn_of(target(d), e)
        whole = p < last
        piece = att.at[p, me_b] if whole else att.at[p, me_b, t]
        sem = b_came.at[p, me_b] if whole else b_last.at[me_b, t]
        pltpu.make_async_remote_copy(
            src_ref=piece, dst_ref=piece, send_sem=b_sent, recv_sem=sem,
            **there(target(d), me_x)).start()

    def spread_in(p, b, t):
        if p < last:
            await_bytes(att.at[p, b], b_came.at[p, b])
        else:
            await_bytes(att.at[p, b, t], b_last.at[b, t])

    def pass_on(p, d, b, t):
        whole = p < last
        piece = att.at[p, b] if whole else att.at[p, b, t]
        sem = b_came.at[p, b] if whole else b_last.at[b, t]
        pltpu.make_async_remote_copy(
            src_ref=piece, dst_ref=piece, send_sem=passed, recv_sem=sem,
            **there(target(d), me_x)).start()

    def spread_near(p):
        for e in range(nb if p == last else 1):
            for d in range(1, side):
                spread(p, d, e)

    def forward(p, t):
        @pl.when(is_gate)
        def _():
            for i in range(side):
                b = far_side + my_side * i + (1 - my_side) * (side - 1 - i)
                spread_in(p, b, t)
                for d in range(1, side):
                    pass_on(p, d, b, t)

    for p in range(pairs):
        with jax.named_scope(f"wA{p}"):
            await_bytes(got.at[p, :, pl.ds(0, m - 1)], a_came.at[p])
        if p == 0:
            for later in range(1, pairs):
                for b in range(nb - 1, 0, -1):
                    when((b > me_b) & (me_b == 0), lambda: ship_level(later, b))
        swap(p).start()
        if p == last:
            for early in range(last):
                when(held, lambda: spread(early, 0, 0))
            forward(0, 0)
        q_all = jnp.concatenate([got[p, 0, i].astype(jnp.float32) for i in range(m)], axis=0)
        q_two = jnp.concatenate(
            [jnp.where(low, q_all, 0.0), jnp.where(low, 0.0, q_all)], axis=0).astype(jnp.bfloat16)
        with jax.named_scope(f"wK{p}"):
            await_bytes(far.at[p], k_came.at[p])
        k_all, v_all = (
            jnp.concatenate(
                [got[p, s, i].astype(jnp.float32) for i in range(m)]
                + [far[p, s - 1, i].astype(jnp.float32) for i in range(m)], axis=0
            ).astype(jnp.bfloat16)
            for s in (1, 2))
        scores = against(q_two, k_all)
        top = jnp.max(scores, axis=1, keepdims=True)
        weights = jnp.exp2((scores - top) * scale)
        total = jnp.sum(weights, axis=1, keepdims=True)
        both = jnp.dot(
            weights.astype(jnp.bfloat16), v_all, preferred_element_type=jnp.float32) / total
        joined = jnp.where(low, both[:mine_rows], both[mine_rows:]).astype(jnp.bfloat16)
        for t in range(nb):
            att[p, me_b, t] = joined[t * block:(t + 1) * block]
        with jax.named_scope(f"sB{p}"):
            if p < last:
                when(jnp.logical_not(held), lambda: spread(p, 0, 0))
                when(is_gate, lambda: spread_near(p))
            else:
                for e in range(nb):
                    spread(p, 0, e)
                for early in range(1 if True else 0, last):
                    forward(early, 0)
                for early in range(last):
                    when(jnp.logical_not(is_gate), lambda: spread_near(early))
                spread_near(p)

    def settle(p, t):
        @pl.when(jnp.logical_not(is_gate))
        def _():
            for i in range(side):
                spread_in(p, far_side + i, t)

        if p == last:
            forward(p, t)
        for d in range(1, side):
            spread_in(p, target(d), t)

    def weight_of(p):
        return jnp.concatenate(
            [w_ref[pl.ds((b * pairs + p) * LANES, LANES)] for b in range(nb)], axis=0)

    with jax.named_scope("wW"):
        await_bytes(w_mine, w_came)
    for p in range(last):
        with jax.named_scope(f"wB{p}"):
            settle(p, 0)
        seen = jnp.concatenate(
            [att[p, b].reshape(mine_rows, LANES) for b in range(nb)], axis=1)
        part = jnp.dot(seen, weight_of(p), preferred_element_type=jnp.float32).reshape(acc.shape)
        if p == 0:
            acc[...] = part
        else:
            acc[...] += part

    def scatter(t, d):
        x = lax.rem(me_x + d, nx)
        pltpu.make_async_remote_copy(
            src_ref=part_send.at[t, x], dst_ref=part_got.at[t, me_x],
            send_sem=r_sent, recv_sem=r_came.at[t, d - 1], **there(me_b, x)).start()

    def reduce(e):
        t = turn_of(me_b, e)
        total = part_f32[t, me_x]
        for d in range(1, nx):
            x = lax.rem(me_x + nx - d, nx)
            with jax.named_scope(f"wR{e}"):
                await_bytes(part_got.at[t, x], r_came.at[t, d - 1])
            total += part_got[t, x].astype(jnp.float32)
        gated = (gain_ref[me_b] * total).astype(jnp.bfloat16)

        @pl.when(me_b == t)
        def _():
            out_ref[t] = gated

        @pl.when(me_b != t)
        def _():
            final_send[t] = gated
            pltpu.make_async_remote_copy(
                src_ref=final_send.at[t], dst_ref=out_ref.at[me_b],
                send_sem=f_sent, recv_sem=f_came, **there(t, me_x)).start()

    for e in range(nb):
        t = turn_of(me_b, e)
        with jax.named_scope(f"wBl{e}"):
            settle(last, t)
        seen = jnp.concatenate([att[last, b, t] for b in range(nb)], axis=1)
        part = jnp.dot(seen, weight_of(last), preferred_element_type=jnp.float32)
        if pairs > 1:
            part += acc[t]
        for x in range(nx):
            one = part[x * rows:(x + 1) * rows]
            part_f32[t, x] = one
            part_send[t, x] = one.astype(jnp.bfloat16)
        for d in range(1, nx):
            scatter(t, d)
        if e >= 4:
            reduce(e - 4)
    for e in range(nb - 4, nb):
        reduce(e)

    with jax.named_scope("wF"):
        await_bytes(out_ref.at[pl.ds(0, nb - 1)], f_came)

    with jax.named_scope("drain"):
        w_swap.wait_send()
        await_bytes(stage.at[pl.ds(0, m - 1)], a_sent)
        await_bytes(far, k_sent)
        await_bytes(att.at[:, pl.ds(0, side)], b_sent)

        @pl.when(is_gate)
        def _():
            await_bytes(att.at[:, pl.ds(0, side * (side - 1))], passed)

        await_bytes(part_send.at[:, pl.ds(0, nx - 1)], r_sent)
        await_bytes(final_send.at[pl.ds(0, nb - 1)], f_sent)


def fused(nb, nu, query, keys, values, out_weight, out_gain):
    nx = nu // 2
    m = nb * nx
    rows, width = query.shape
    pairs = width // LANES // m
    depth, columns = out_weight.shape
    bf16, f32 = jnp.bfloat16, jnp.float32
    vmem, dma = pltpu.VMEM, pltpu.SemaphoreType.DMA
    in_hbm = pl.BlockSpec(memory_space=pltpu.HBM)
    block = nx * rows
    gathered = pl.pallas_call(
        functools.partial(attend_kernel, nb, nu),
        out_shape=vmem((nb, rows, columns), bf16),
        in_specs=[in_hbm] * 5,
        out_specs=pl.BlockSpec(memory_space=pltpu.VMEM),
        scratch_shapes=[
            vmem((3, rows, width), bf16),
            vmem((nb, 1, columns), f32),
            vmem((m, pairs, 3, rows, LANES), bf16),
            vmem((pairs, 3, m, rows, LANES), bf16),
            vmem((pairs, 2, m, rows, LANES), bf16),
            vmem((2 * depth, columns), bf16),
            vmem((pairs, nb, nb, block, LANES), bf16),
            vmem((nb, block, columns), f32),
            vmem((nb, nx, rows, columns), f32),
            vmem((nb, nx, rows, columns), bf16),
            vmem((nb, nx, rows, columns), bf16),
            vmem((nb, rows, columns), bf16),
            dma, dma, dma, dma, dma, dma((pairs,)), dma, dma((pairs,)),
            pltpu.SemaphoreType.REGULAR((nb - 1,)),
            dma, dma((pairs, nb)), dma((nb, nb)), dma, dma, dma((nb, nx - 1)), dma, dma,
        ],
        compiler_params=pltpu.CompilerParams(
            collective_id=0, has_side_effects=True),
    )(query, keys, values, out_weight, out_gain.reshape(nb, 1, columns))
    return gathered.transpose(1, 0, 2).reshape(rows, width)


def on_any(nb, nu, query, keys, values, out_weight, out_gain):
    rows, width = query.shape
    suits = (
        nu % 2 == 0 and nu > 2 and nb % 2 == 0 and width % (LANES * nb * nu // 2) == 0
        and rows % 8 == 0 and (nu // 2 * rows) % 16 == 0 and (width // nb) % LANES == 0
    )
    plan = functools.partial(fused, nb, nu) if suits else on_device
    return plan(query, keys, values, out_weight, out_gain)


def solution(mesh):
    in_specs = (
        P(("group", "blk", "uly"), None),
        P(("group", "blk", "uly"), None),
        P(("group", "blk", "uly"), None),
        P("uly", "blk"),
        P(),
    )
    out_specs = P(("group", "blk", "uly"), None)
    body = functools.partial(on_any, mesh.shape["blk"], mesh.shape["uly"])
    return jax.shard_map(
        body, mesh=mesh, in_specs=in_specs, out_specs=out_specs, check_vma=False
    )
```

```python
import functools
import math

import jax
import jax.numpy as jnp
from jax import lax
from jax.experimental import pallas as pl
from jax.experimental.pallas import tpu as pltpu
from jax.sharding import PartitionSpec as P

HEAD = 64
LANES = 128
MESH = pl.DeviceIdType.MESH

def make_fold(query_heads, state_now, pieces):
    score_scale = 1.0 / math.sqrt(HEAD)
    head_count = query_heads.shape[1]
    running_max, denominator, weighted = state_now
    key_part, value_part = pieces
    key_count = key_part.shape[0]
    key_heads = key_part.reshape(key_count, head_count, HEAD)
    value_heads = value_part.reshape(key_count, head_count, HEAD)
    scores = (
        jnp.einsum("qhd,khd->qhk", query_heads, key_heads, preferred_element_type=jnp.float32)
        * score_scale
    )
    new_max = jnp.max(scores, axis=2)
    weights = jnp.exp(scores - new_max[:, :, None])
    shrink = jnp.exp(running_max - new_max)
    denominator = denominator * shrink + jnp.sum(weights, axis=2)
    weighted = weighted * shrink[:, :, None] + jnp.einsum(
        "qhk,khd->qhd",
        weights.astype(jnp.bfloat16),
        value_heads,
        preferred_element_type=jnp.float32,
    )
    return (new_max, denominator, weighted)


def initial_state(row_count, head_count):
    return (
        jnp.full((row_count, head_count), -jnp.inf, jnp.float32),
        jnp.zeros((row_count, head_count), jnp.float32),
        jnp.zeros((row_count, head_count, HEAD), jnp.float32),
    )


def on_device(query, keys, values, out_weight, out_gain):
    grouped_q, grouped_k, grouped_v = (
        lax.all_to_all(query, "uly", split_axis=1, concat_axis=0, tiled=True),
        lax.all_to_all(keys, "uly", split_axis=1, concat_axis=0, tiled=True),
        lax.all_to_all(values, "uly", split_axis=1, concat_axis=0, tiled=True),
    )
    row_count = grouped_q.shape[0]
    features = grouped_q.shape[1]
    local_heads = features // HEAD
    query_heads = grouped_q.reshape(row_count, local_heads, HEAD)
    half_heads = local_heads // 2
    half_width = half_heads * HEAD
    low_state = make_fold(
        query_heads[:, :half_heads],
        initial_state(row_count, half_heads),
        (
            lax.all_gather(grouped_k[:, :half_width], "blk", axis=0, tiled=True),
            lax.all_gather(grouped_v[:, :half_width], "blk", axis=0, tiled=True),
        ),
    )
    high_state = make_fold(
        query_heads[:, half_heads:],
        initial_state(row_count, local_heads - half_heads),
        (
            lax.all_gather(grouped_k[:, half_width:], "blk", axis=0, tiled=True),
            lax.all_gather(grouped_v[:, half_width:], "blk", axis=0, tiled=True),
        ),
    )
    denominator = jnp.concatenate([low_state[1], high_state[1]], axis=1)
    weighted = jnp.concatenate([low_state[2], high_state[2]], axis=1)
    attended = (
        (weighted / denominator[:, :, None]).reshape(row_count, features).astype(jnp.bfloat16)
    )
    partial_value = jnp.dot(
        attended,
        lax.all_gather(out_weight, "blk", axis=1, tiled=True),
        preferred_element_type=jnp.float32,
    )
    summed = lax.psum_scatter(
        partial_value.astype(jnp.bfloat16), "uly", scatter_dimension=0, tiled=True
    ).astype(jnp.float32)
    return (out_gain * summed).astype(jnp.bfloat16)


def attend_kernel(
    nb, nu,
    q_hbm, k_hbm, v_hbm, w_hbm, gain_hbm, out_ref,
    qkv_ref, gain_ref, stage, got, far, w_ref,
    att, acc, part_f32, part_send, part_got, final_send,
    in_sem, w_in, w_sent, w_came, a_sent, a_came, k_sent, k_came, up_sem,
    b_sent, b_came, b_last, passed, r_sent, r_came, f_sent, f_came,
):
    nx = nu // 2
    m = nb * nx
    rows, width = q_hbm.shape
    pairs = stage.shape[1]
    last = pairs - 1
    depth = w_hbm.shape[0]
    block = nx * rows
    mine_rows = nb * block
    side = nb // 2
    scale = math.log2(math.e) / math.sqrt(HEAD)
    me_b, me_u = lax.axis_index("blk"), lax.axis_index("uly")
    me_x, me_c = me_u // 2, lax.rem(me_u, 2)
    me = me_b * nx + me_x
    my_side = me_b // side
    gate_here = (side - 1) + my_side
    gate_there = side - my_side
    is_gate = me_b == gate_here
    held = me_b < 0
    far_side = (1 - my_side) * side

    def turn_of(b, e):
        upward = b // side
        return upward * e + (1 - upward) * (nb - 1 - e)

    def there(b, x):
        return dict(device_id={"blk": b, "uly": 2 * x + me_c}, device_id_type=MESH)

    partner = dict(device_id={"blk": me_b, "uly": 2 * me_x + 1 - me_c}, device_id_type=MESH)

    def await_bytes(ref, sem):
        pltpu.make_async_copy(ref, ref, sem).wait()

    def when(condition, action):
        pl.when(condition)(action)

    barrier = pltpu.get_barrier_semaphore()
    pl.semaphore_signal(barrier, inc=1, **partner)
    for d in range(1, nx):
        pl.semaphore_signal(barrier, inc=1, **there(me_b, lax.rem(me_x + d, nx)))
    for b in range(1, nb):

        @pl.when(b > me_b)
        def _():
            for x in range(nx):
                pl.semaphore_signal(barrier, inc=1, **there(b, x))

    for s, ref in enumerate((q_hbm, k_hbm, v_hbm)):
        pltpu.make_async_copy(ref, qkv_ref.at[s], in_sem).start()
    w_mine = w_ref.at[pl.ds(pl.multiple_of(me_c * depth, depth), depth)]
    with jax.named_scope("barrier"):
        pl.semaphore_wait(barrier, me_b * nx + nx)
    for b in range(nb - 1):

        @pl.when(b < me_b)
        def _():
            for x in range(nx):
                pl.semaphore_signal(up_sem.at[me_b - 1], inc=1, **there(b, x))

    with jax.named_scope("load"):
        await_bytes(qkv_ref, in_sem)
    w_load = pltpu.make_async_copy(w_hbm, w_mine, w_in)
    gain_load = pltpu.make_async_copy(gain_hbm, gain_ref, in_sem)
    w_load.start()
    gain_load.start()

    for b in range(nb):
        for x in range(nx):
            for p in range(pairs):
                at = ((x * nb + b) * pairs + p) * LANES
                for s in range(3):
                    stage[b * nx + x, p, s] = qkv_ref[s, :, pl.ds(at, LANES)]
    for p in range(pairs):
        for s in range(3):
            got[p, s, me] = stage[me, p, s]


    def ship(p, b, x):
        pltpu.make_async_remote_copy(
            src_ref=stage.at[b * nx + x, p], dst_ref=got.at[p, :, me],
            send_sem=a_sent, recv_sem=a_came.at[p], **there(b, x)).start()

    def ship_level(p, b):
        for d in range(nx - 1, -1, -1):
            ship(p, b, lax.rem(me_x + d, nx))

    def ship_beside(p):
        for d in range(1, nx):
            ship(p, me_b, lax.rem(me_x + d, nx))

    for p in range(pairs):
        for b in range(nb - 1):
            when(b < me_b, lambda: ship_level(p, b))
        ship_beside(p)

    w_swap = pltpu.make_async_remote_copy(
        src_ref=w_mine, dst_ref=w_mine, send_sem=w_sent, recv_sem=w_came, **partner)
    w_load.wait()
    gain_load.wait()
    w_swap.start()

    for b in range(1, nb):

        @pl.when(b > me_b)
        def _():
            with jax.named_scope(f"up{b}"):
                pl.semaphore_wait(up_sem.at[b - 1], nx)
            ship_level(0, b)
    for p in range(1, pairs):
        for b in range(nb - 1, 0, -1):
            when((b > me_b) & ((me_b > 0) | (b == 1)), lambda: ship_level(p, b))

    def swap(p):
        return pltpu.make_async_remote_copy(
            src_ref=got.at[p, pl.ds(1, 2)], dst_ref=far.at[p],
            send_sem=k_sent, recv_sem=k_came.at[p], **partner)

    def against(a, b):
        return lax.dot_general(a, b, (((1,), (1,)), ((), ())), preferred_element_type=jnp.float32)

    low = lax.broadcasted_iota(jnp.int32, (mine_rows, LANES), 1) < HEAD

    def target(d):
        return gate_there if d == 0 else my_side * side + lax.rem(me_b + d, side)

    def came(p, b, t):
        return b_came.at[p, b] if t is None else b_last.at[b, t]

    def piece(p, b, t):
        return att.at[p, b] if t is None else att.at[p, b, t]

    def push(p, d, b, t, sent, sem):
        pltpu.make_async_remote_copy(
            src_ref=piece(p, b, t), dst_ref=piece(p, b, t), send_sem=sent, recv_sem=sem,
            **there(target(d), me_x)).start()

    def spread(p, d):
        if p < last:
            push(p, d, me_b, None, b_sent, came(p, me_b, None))
        else:
            for e in range(nb):
                t = turn_of(target(d), e)
                push(p, d, me_b, t, b_sent, came(p, me_b, t))

    def spread_near(p):
        for d in range(1, side):
            spread(p, d)

    def far_of(i):
        return far_side + my_side * i + (1 - my_side) * (side - 1 - i)

    def near_of(d):
        return my_side * side + lax.rem(me_b + d, side)

    upper = my_side == 1
    late_core = (me_b < side) & (me_c == 1)

    def forward(p, turns, whose, fresh=True, only=True):
        @pl.when(is_gate & only)
        def _():
            for e in turns:
                t = turn_of(me_b, e)
                for i in whose:
                    b = far_of(i)
                    if p == last:
                        await_bytes(att.at[p, b, t], b_last.at[b, t])
                    elif fresh and e == turns[0]:
                        await_bytes(att.at[p, b], b_came.at[p, b])
                    for d in range(1, side):
                        push(p, d, b, t, passed, came(p, b, t))

    every = list(range(side))
    head, tail = range(nb - 1), range(nb - 1, nb)

    for p in range(pairs):
        with jax.named_scope(f"wA{p}"):
            await_bytes(got.at[p, :, pl.ds(0, m - 1)], a_came.at[p])
        if p == 0:
            for later in range(1, min(2, pairs)):
                for b in range(nb - 1, 1, -1):
                    when(me_b == 0, lambda: ship_level(later, b))
        swap(p).start()
        if p == last:
            for early in range(last):
                when(held, lambda: spread(early, 0))
        q_all = jnp.concatenate([got[p, 0, i].astype(jnp.float32) for i in range(m)], axis=0)
        q_two = jnp.concatenate(
            [jnp.where(low, q_all, 0.0), jnp.where(low, 0.0, q_all)], axis=0).astype(jnp.bfloat16)
        with jax.named_scope(f"wK{p}"):
            await_bytes(far.at[p], k_came.at[p])
        if p == last and last > 0:
            when(late_core, lambda: spread(last - 1, 0))
        k_all, v_all = (
            jnp.concatenate(
                [got[p, s, i].astype(jnp.float32) for i in range(m)]
                + [far[p, s - 1, i].astype(jnp.float32) for i in range(m)], axis=0
            ).astype(jnp.bfloat16)
            for s in (1, 2))
        scores = against(q_two, k_all)
        top = jnp.max(scores, axis=1, keepdims=True)
        weights = jnp.exp2((scores - top) * scale)
        total = jnp.sum(weights, axis=1, keepdims=True)
        both = jnp.dot(
            weights.astype(jnp.bfloat16), v_all, preferred_element_type=jnp.float32) / total
        joined = jnp.where(low, both[:mine_rows], both[mine_rows:]).astype(jnp.bfloat16)
        for t in range(nb):
            att[p, me_b, t] = joined[t * block:(t + 1) * block]
        with jax.named_scope(f"sB{p}"):
            if p < last:
                when(jnp.logical_not(held | (late_core & (p == last - 1))), lambda: spread(p, 0))
                if p == 0:
                    for later in range(2, pairs):
                        for b in range(nb - 1, 1, -1):
                            when(me_b == 0, lambda: ship_level(later, b))
                when(is_gate, lambda: spread_near(p))
                if p == last - 1:
                    for early, i in ((0, 0),):
                        with jax.named_scope(f"fa{early}{i}"):
                            forward(early, head, [i], only=upper)
            else:
                spread(p, 0)
                for early in range(last):
                    with jax.named_scope(f"fw{early}"):
                        for i in every:
                            if (early, i) in ((0, 0),):
                                forward(early, head, [i], only=jnp.logical_not(upper))
                            else:
                                forward(early, head, [i])
                for early in range(last):
                    when(jnp.logical_not(is_gate), lambda: spread_near(early))
                spread_near(p)
                with jax.named_scope(f"fwl"):
                    forward(last, head, every)
                for early in range(last):
                    forward(early, tail, every, fresh=False)
                with jax.named_scope(f"fwm"):
                    forward(last, tail, every)

    def weight_of(p, b):
        at = pl.multiple_of((b * pairs + p) * LANES, LANES)
        return w_ref[pl.ds(at, LANES)]

    beside = [near_of(d) for d in range(side)]
    across = [far_side + i for i in range(side)]

    with jax.named_scope("wW"):
        await_bytes(w_mine, w_came)
    for p in range(last):
        for d in range(1, side):
            with jax.named_scope(f"wB{p}"):
                await_bytes(att.at[p, beside[d]], b_came.at[p, beside[d]])
    if last:
        early = [(p, b) for p in range(last) for b in beside]
        seen = jnp.concatenate([att[p, b].reshape(mine_rows, LANES) for p, b in early], axis=1)
        weight = jnp.concatenate([weight_of(p, b) for p, b in early], axis=0)
        acc[...] = jnp.dot(seen, weight, preferred_element_type=jnp.float32).reshape(acc.shape)
    late = [(p, b) for p in range(pairs) for b in across] + [(last, b) for b in beside]

    def scatter(t, d):
        x = lax.rem(me_x + d, nx)
        pltpu.make_async_remote_copy(
            src_ref=part_send.at[t, x], dst_ref=part_got.at[t, me_x],
            send_sem=r_sent, recv_sem=r_came.at[t, d - 1], **there(me_b, x)).start()

    def reduce(e):
        t = turn_of(me_b, e)
        total = part_f32[t, me_x]
        for d in range(1, nx):
            x = lax.rem(me_x + nx - d, nx)
            with jax.named_scope(f"wR{e}"):
                await_bytes(part_got.at[t, x], r_came.at[t, d - 1])
            total += part_got[t, x].astype(jnp.float32)
        gated = (gain_ref[me_b] * total).astype(jnp.bfloat16)

        @pl.when(me_b == t)
        def _():
            out_ref[t] = gated

        @pl.when(me_b != t)
        def _():
            final_send[t] = gated
            pltpu.make_async_remote_copy(
                src_ref=final_send.at[t], dst_ref=out_ref.at[me_b],
                send_sem=f_sent, recv_sem=f_came, **there(t, me_x)).start()

    for e in range(nb):
        t = turn_of(me_b, e)
        with jax.named_scope(f"wBl{e}"):
            @pl.when(jnp.logical_not(is_gate))
            def _():
                for b in across:
                    await_bytes(att.at[:, b, t], b_last.at[b, t])

            for d in range(1, side):
                await_bytes(att.at[last, beside[d], t], b_last.at[beside[d], t])
        seen = jnp.concatenate([att[p, b, t] for p, b in late], axis=1)
        weight = jnp.concatenate([weight_of(p, b) for p, b in late], axis=0)
        part = jnp.dot(seen, weight, preferred_element_type=jnp.float32)
        if last:
            part += acc[t]
        for x in range(nx):
            one = part[x * rows:(x + 1) * rows]
            part_f32[t, x] = one
            part_send[t, x] = one.astype(jnp.bfloat16)
        for d in range(1, nx):
            scatter(t, d)
        if e >= 4:
            reduce(e - 4)
    for e in range(nb - 4, nb):
        reduce(e)

    with jax.named_scope("wF"):
        await_bytes(out_ref.at[pl.ds(0, nb - 1)], f_came)

    with jax.named_scope("drain"):
        w_swap.wait_send()
        await_bytes(stage.at[pl.ds(0, m - 1)], a_sent)
        await_bytes(far, k_sent)
        await_bytes(att.at[:, pl.ds(0, side)], b_sent)

        @pl.when(is_gate)
        def _():
            await_bytes(att.at[:, pl.ds(0, side * (side - 1))], passed)

        await_bytes(part_send.at[:, pl.ds(0, nx - 1)], r_sent)
        await_bytes(final_send.at[pl.ds(0, nb - 1)], f_sent)


def fused(nb, nu, query, keys, values, out_weight, out_gain):
    nx = nu // 2
    m = nb * nx
    rows, width = query.shape
    pairs = width // LANES // m
    depth, columns = out_weight.shape
    bf16, f32 = jnp.bfloat16, jnp.float32
    vmem, dma = pltpu.VMEM, pltpu.SemaphoreType.DMA
    in_hbm = pl.BlockSpec(memory_space=pltpu.HBM)
    block = nx * rows
    gathered = pl.pallas_call(
        functools.partial(attend_kernel, nb, nu),
        out_shape=vmem((nb, rows, columns), bf16),
        in_specs=[in_hbm] * 5,
        out_specs=pl.BlockSpec(memory_space=pltpu.VMEM),
        scratch_shapes=[
            vmem((3, rows, width), bf16),
            vmem((nb, 1, columns), f32),
            vmem((m, pairs, 3, rows, LANES), bf16),
            vmem((pairs, 3, m, rows, LANES), bf16),
            vmem((pairs, 2, m, rows, LANES), bf16),
            vmem((2 * depth, columns), bf16),
            vmem((pairs, nb, nb, block, LANES), bf16),
            vmem((nb, block, columns), f32),
            vmem((nb, nx, rows, columns), f32),
            vmem((nb, nx, rows, columns), bf16),
            vmem((nb, nx, rows, columns), bf16),
            vmem((nb, rows, columns), bf16),
            dma, dma, dma, dma, dma, dma((pairs,)), dma, dma((pairs,)),
            pltpu.SemaphoreType.REGULAR((nb - 1,)),
            dma, dma((pairs, nb)), dma((nb, nb)), dma, dma, dma((nb, nx - 1)), dma, dma,
        ],
        compiler_params=pltpu.CompilerParams(
            collective_id=0, has_side_effects=True),
    )(query, keys, values, out_weight, out_gain.reshape(nb, 1, columns))
    return gathered.transpose(1, 0, 2).reshape(rows, width)


def on_any(nb, nu, query, keys, values, out_weight, out_gain):
    rows, width = query.shape
    suits = (
        nu % 2 == 0 and nu > 2 and nb % 2 == 0 and width % (LANES * nb * nu // 2) == 0
        and rows % 8 == 0 and (nu // 2 * rows) % 16 == 0 and (width // nb) % LANES == 0
    )
    plan = functools.partial(fused, nb, nu) if suits else on_device
    return plan(query, keys, values, out_weight, out_gain)


def solution(mesh):
    in_specs = (
        P(("group", "blk", "uly"), None),
        P(("group", "blk", "uly"), None),
        P(("group", "blk", "uly"), None),
        P("uly", "blk"),
        P(),
    )
    out_specs = P(("group", "blk", "uly"), None)
    body = functools.partial(on_any, mesh.shape["blk"], mesh.shape["uly"])
    return jax.shard_map(
        body, mesh=mesh, in_specs=in_specs, out_specs=out_specs, check_vma=False
    )
```

```python
import functools
import math

import jax
import jax.numpy as jnp
from jax import lax
from jax.experimental import pallas as pl
from jax.experimental.pallas import tpu as pltpu
from jax.sharding import PartitionSpec as P

HEAD = 64
LANES = 128
MESH = pl.DeviceIdType.MESH

def make_fold(query_heads, state_now, pieces):
    score_scale = 1.0 / math.sqrt(HEAD)
    head_count = query_heads.shape[1]
    running_max, denominator, weighted = state_now
    key_part, value_part = pieces
    key_count = key_part.shape[0]
    key_heads = key_part.reshape(key_count, head_count, HEAD)
    value_heads = value_part.reshape(key_count, head_count, HEAD)
    scores = (
        jnp.einsum("qhd,khd->qhk", query_heads, key_heads, preferred_element_type=jnp.float32)
        * score_scale
    )
    new_max = jnp.max(scores, axis=2)
    weights = jnp.exp(scores - new_max[:, :, None])
    shrink = jnp.exp(running_max - new_max)
    denominator = denominator * shrink + jnp.sum(weights, axis=2)
    weighted = weighted * shrink[:, :, None] + jnp.einsum(
        "qhk,khd->qhd",
        weights.astype(jnp.bfloat16),
        value_heads,
        preferred_element_type=jnp.float32,
    )
    return (new_max, denominator, weighted)


def initial_state(row_count, head_count):
    return (
        jnp.full((row_count, head_count), -jnp.inf, jnp.float32),
        jnp.zeros((row_count, head_count), jnp.float32),
        jnp.zeros((row_count, head_count, HEAD), jnp.float32),
    )


def on_device(query, keys, values, out_weight, out_gain):
    grouped_q, grouped_k, grouped_v = (
        lax.all_to_all(query, "uly", split_axis=1, concat_axis=0, tiled=True),
        lax.all_to_all(keys, "uly", split_axis=1, concat_axis=0, tiled=True),
        lax.all_to_all(values, "uly", split_axis=1, concat_axis=0, tiled=True),
    )
    row_count = grouped_q.shape[0]
    features = grouped_q.shape[1]
    local_heads = features // HEAD
    query_heads = grouped_q.reshape(row_count, local_heads, HEAD)
    half_heads = local_heads // 2
    half_width = half_heads * HEAD
    low_state = make_fold(
        query_heads[:, :half_heads],
        initial_state(row_count, half_heads),
        (
            lax.all_gather(grouped_k[:, :half_width], "blk", axis=0, tiled=True),
            lax.all_gather(grouped_v[:, :half_width], "blk", axis=0, tiled=True),
        ),
    )
    high_state = make_fold(
        query_heads[:, half_heads:],
        initial_state(row_count, local_heads - half_heads),
        (
            lax.all_gather(grouped_k[:, half_width:], "blk", axis=0, tiled=True),
            lax.all_gather(grouped_v[:, half_width:], "blk", axis=0, tiled=True),
        ),
    )
    denominator = jnp.concatenate([low_state[1], high_state[1]], axis=1)
    weighted = jnp.concatenate([low_state[2], high_state[2]], axis=1)
    attended = (
        (weighted / denominator[:, :, None]).reshape(row_count, features).astype(jnp.bfloat16)
    )
    partial_value = jnp.dot(
        attended,
        lax.all_gather(out_weight, "blk", axis=1, tiled=True),
        preferred_element_type=jnp.float32,
    )
    summed = lax.psum_scatter(
        partial_value.astype(jnp.bfloat16), "uly", scatter_dimension=0, tiled=True
    ).astype(jnp.float32)
    return (out_gain * summed).astype(jnp.bfloat16)


def attend_kernel(
    nb, nu,
    q_hbm, k_hbm, v_hbm, w_hbm, gain_hbm, out_ref,
    qkv_ref, gain_ref, stage, got, far, w_ref,
    att, acc, part_f32, part_send, part_got, final_send,
    in_sem, w_in, w_sent, w_came, a_sent, a_came, k_sent, k_came, up_sem,
    b_sent, b_came, b_last, passed, r_sent, r_came, f_sent, f_came,
):
    nx = nu // 2
    m = nb * nx
    rows, width = q_hbm.shape
    pairs = stage.shape[1]
    last = pairs - 1
    depth = w_hbm.shape[0]
    block = nx * rows
    mine_rows = nb * block
    side = nb // 2
    scale = math.log2(math.e) / math.sqrt(HEAD)
    me_b, me_u = lax.axis_index("blk"), lax.axis_index("uly")
    me_x, me_c = me_u // 2, lax.rem(me_u, 2)
    me = me_b * nx + me_x
    my_side = me_b // side
    gate_here = (side - 1) + my_side
    gate_there = side - my_side
    is_gate = me_b == gate_here
    held = me_b < 0
    far_side = (1 - my_side) * side

    def turn_of(b, e):
        upward = b // side
        return upward * e + (1 - upward) * (nb - 1 - e)

    def order_here(e):
        if e == nb - 1:
            return me_b
        down = nb - 1 - e
        return my_side * (e + (e >= me_b)) + (1 - my_side) * (down - (down <= me_b))

    def there(b, x):
        return dict(device_id={"blk": b, "uly": 2 * x + me_c}, device_id_type=MESH)

    partner = dict(device_id={"blk": me_b, "uly": 2 * me_x + 1 - me_c}, device_id_type=MESH)

    def await_bytes(ref, sem):
        pltpu.make_async_copy(ref, ref, sem).wait()

    def when(condition, action):
        pl.when(condition)(action)

    barrier = pltpu.get_barrier_semaphore()
    pl.semaphore_signal(barrier, inc=1, **partner)
    for d in range(1, nx):
        pl.semaphore_signal(barrier, inc=1, **there(me_b, lax.rem(me_x + d, nx)))
    for b in range(1, nb):

        @pl.when(b > me_b)
        def _():
            for x in range(nx):
                pl.semaphore_signal(barrier, inc=1, **there(b, x))

    for s, ref in enumerate((q_hbm, k_hbm, v_hbm)):
        pltpu.make_async_copy(ref, qkv_ref.at[s], in_sem).start()
    w_mine = w_ref.at[pl.ds(pl.multiple_of(me_c * depth, depth), depth)]
    with jax.named_scope("barrier"):
        pl.semaphore_wait(barrier, me_b * nx + nx)
    for b in range(nb - 1):

        @pl.when(b < me_b)
        def _():
            for x in range(nx):
                pl.semaphore_signal(up_sem.at[me_b - 1], inc=1, **there(b, x))

    with jax.named_scope("load"):
        await_bytes(qkv_ref, in_sem)
    w_load = pltpu.make_async_copy(w_hbm, w_mine, w_in)
    gain_load = pltpu.make_async_copy(gain_hbm, gain_ref, in_sem)
    w_load.start()
    gain_load.start()

    for b in range(nb):
        for x in range(nx):
            for p in range(pairs):
                at = ((x * nb + b) * pairs + p) * LANES
                for s in range(3):
                    stage[b * nx + x, p, s] = qkv_ref[s, :, pl.ds(at, LANES)]
    for p in range(pairs):
        for s in range(3):
            got[p, s, me] = stage[me, p, s]


    def ship(p, b, x):
        pltpu.make_async_remote_copy(
            src_ref=stage.at[b * nx + x, p], dst_ref=got.at[p, :, me],
            send_sem=a_sent, recv_sem=a_came.at[p], **there(b, x)).start()

    def ship_level(p, b):
        for d in range(nx - 1, -1, -1):
            ship(p, b, lax.rem(me_x + d, nx))

    def ship_beside(p):
        for d in range(1, nx):
            ship(p, me_b, lax.rem(me_x + d, nx))

    for p in range(pairs):
        for b in range(nb - 1):
            when(b < me_b, lambda: ship_level(p, b))
        ship_beside(p)

    w_swap = pltpu.make_async_remote_copy(
        src_ref=w_mine, dst_ref=w_mine, send_sem=w_sent, recv_sem=w_came, **partner)
    w_load.wait()
    gain_load.wait()
    w_swap.start()

    for b in range(1, nb):

        @pl.when(b > me_b)
        def _():
            with jax.named_scope(f"up{b}"):
                pl.semaphore_wait(up_sem.at[b - 1], nx)
            ship_level(0, b)
    for p in range(1, pairs):
        for b in range(nb - 1, 0, -1):
            when((b > me_b) & ((me_b > 0) | (b == 1)), lambda: ship_level(p, b))

    def swap(p):
        return pltpu.make_async_remote_copy(
            src_ref=got.at[p, pl.ds(1, 2)], dst_ref=far.at[p],
            send_sem=k_sent, recv_sem=k_came.at[p], **partner)

    def against(a, b):
        return lax.dot_general(a, b, (((1,), (1,)), ((), ())), preferred_element_type=jnp.float32)

    low = lax.broadcasted_iota(jnp.int32, (mine_rows, LANES), 1) < HEAD

    def target(d):
        return gate_there if d == 0 else my_side * side + lax.rem(me_b + d, side)

    def came(p, b, t):
        return b_came.at[p, b] if t is None else b_last.at[b, t]

    def piece(p, b, t):
        return att.at[p, b] if t is None else att.at[p, b, t]

    def push(p, d, b, t, sent, sem):
        pltpu.make_async_remote_copy(
            src_ref=piece(p, b, t), dst_ref=piece(p, b, t), send_sem=sent, recv_sem=sem,
            **there(target(d), me_x)).start()

    def spread(p, d):
        if p < last:
            push(p, d, me_b, None, b_sent, came(p, me_b, None))
        else:
            for e in range(nb):
                t = turn_of(target(d), e)
                push(p, d, me_b, t, b_sent, came(p, me_b, t))

    def spread_near(p):
        for d in range(1, side):
            spread(p, d)

    def far_of(i):
        return far_side + my_side * i + (1 - my_side) * (side - 1 - i)

    def near_of(d):
        return my_side * side + lax.rem(me_b + d, side)

    upper = my_side == 1
    late_core = (me_b < side) & (me_c == 1)

    def forward(p, turns, whose, fresh=True, only=True):
        @pl.when(is_gate & only)
        def _():
            for e in turns:
                t = turn_of(me_b, e)
                for i in whose:
                    b = far_of(i)
                    if p == last:
                        await_bytes(att.at[p, b, t], b_last.at[b, t])
                    elif fresh and e == turns[0]:
                        await_bytes(att.at[p, b], b_came.at[p, b])
                    for d in range(1, side):
                        push(p, d, b, t, passed, came(p, b, t))

    every = list(range(side))
    head, tail = range(nb - 1), range(nb - 1, nb)

    for p in range(pairs):
        with jax.named_scope(f"wA{p}"):
            await_bytes(got.at[p, :, pl.ds(0, m - 1)], a_came.at[p])
        if p == 0:
            for later in range(1, min(2, pairs)):
                for b in range(nb - 1, 1, -1):
                    when(me_b == 0, lambda: ship_level(later, b))
        swap(p).start()
        if p == last:
            for early in range(last):
                when(held, lambda: spread(early, 0))
        q_all = jnp.concatenate([got[p, 0, i].astype(jnp.float32) for i in range(m)], axis=0)
        q_two = jnp.concatenate(
            [jnp.where(low, q_all, 0.0), jnp.where(low, 0.0, q_all)], axis=0).astype(jnp.bfloat16)
        with jax.named_scope(f"wK{p}"):
            await_bytes(far.at[p], k_came.at[p])
        if p == last and last > 0:
            when(late_core, lambda: spread(last - 1, 0))
        k_all, v_all = (
            jnp.concatenate(
                [got[p, s, i].astype(jnp.float32) for i in range(m)]
                + [far[p, s - 1, i].astype(jnp.float32) for i in range(m)], axis=0
            ).astype(jnp.bfloat16)
            for s in (1, 2))
        scores = against(q_two, k_all)
        top = jnp.max(scores, axis=1, keepdims=True)
        weights = jnp.exp2((scores - top) * scale)
        total = jnp.sum(weights, axis=1, keepdims=True)
        both = jnp.dot(
            weights.astype(jnp.bfloat16), v_all, preferred_element_type=jnp.float32) / total
        joined = jnp.where(low, both[:mine_rows], both[mine_rows:]).astype(jnp.bfloat16)
        for t in range(nb):
            att[p, me_b, t] = joined[t * block:(t + 1) * block]
        with jax.named_scope(f"sB{p}"):
            if p < last:
                when(jnp.logical_not(held | (late_core & (p == last - 1))), lambda: spread(p, 0))
                if p == 0:
                    for later in range(2, pairs):
                        for b in range(nb - 1, 1, -1):
                            when(me_b == 0, lambda: ship_level(later, b))
                when(is_gate, lambda: spread_near(p))
                if p == last - 1:
                    for early, i in ((0, 0),):
                        with jax.named_scope(f"fa{early}{i}"):
                            forward(early, head, [i], only=upper)
            else:
                spread(p, 0)
                for early in range(last):
                    with jax.named_scope(f"fw{early}"):
                        for i in every:
                            if (early, i) in ((0, 0),):
                                forward(early, head, [i], only=jnp.logical_not(upper))
                            else:
                                forward(early, head, [i])
                for early in range(last):
                    when(jnp.logical_not(is_gate), lambda: spread_near(early))
                spread_near(p)
                with jax.named_scope(f"fwl"):
                    forward(last, head, every)
                for early in range(last):
                    forward(early, tail, every, fresh=False)
                with jax.named_scope(f"fwm"):
                    forward(last, tail, every)

    def weight_of(p, b):
        at = pl.multiple_of((b * pairs + p) * LANES, LANES)
        return w_ref[pl.ds(at, LANES)]

    beside = [near_of(d) for d in range(side)]
    across = [far_side + i for i in range(side)]

    with jax.named_scope("wW"):
        await_bytes(w_mine, w_came)
    for p in range(last):
        for d in range(1, side):
            with jax.named_scope(f"wB{p}"):
                await_bytes(att.at[p, beside[d]], b_came.at[p, beside[d]])
    if last:
        early = [(p, b) for p in range(last) for b in beside]
        seen = jnp.concatenate([att[p, b].reshape(mine_rows, LANES) for p, b in early], axis=1)
        weight = jnp.concatenate([weight_of(p, b) for p, b in early], axis=0)
        acc[...] = jnp.dot(seen, weight, preferred_element_type=jnp.float32).reshape(acc.shape)
    late = [(p, b) for p in range(pairs) for b in across] + [(last, b) for b in beside]

    def scatter(t, d):
        x = lax.rem(me_x + d, nx)
        pltpu.make_async_remote_copy(
            src_ref=part_send.at[t, x], dst_ref=part_got.at[t, me_x],
            send_sem=r_sent, recv_sem=r_came.at[t, d - 1], **there(me_b, x)).start()

    def reduce(e):
        t = order_here(e)
        total = part_f32[t, me_x]
        for d in range(1, nx):
            x = lax.rem(me_x + nx - d, nx)
            with jax.named_scope(f"wR{e}"):
                await_bytes(part_got.at[t, x], r_came.at[t, d - 1])
            total += part_got[t, x].astype(jnp.float32)
        gated = (gain_ref[me_b] * total).astype(jnp.bfloat16)

        @pl.when(me_b == t)
        def _():
            out_ref[t] = gated

        @pl.when(me_b != t)
        def _():
            final_send[t] = gated
            pltpu.make_async_remote_copy(
                src_ref=final_send.at[t], dst_ref=out_ref.at[me_b],
                send_sem=f_sent, recv_sem=f_came, **there(t, me_x)).start()

    for e in range(nb):
        t = order_here(e)
        with jax.named_scope(f"wBl{e}"):
            @pl.when(jnp.logical_not(is_gate))
            def _():
                for b in across:
                    await_bytes(att.at[:, b, t], b_last.at[b, t])

            for d in range(1, side):
                await_bytes(att.at[last, beside[d], t], b_last.at[beside[d], t])
        seen = jnp.concatenate([att[p, b, t] for p, b in late], axis=1)
        weight = jnp.concatenate([weight_of(p, b) for p, b in late], axis=0)
        part = jnp.dot(seen, weight, preferred_element_type=jnp.float32)
        if last:
            part += acc[t]
        for x in range(nx):
            one = part[x * rows:(x + 1) * rows]
            part_f32[t, x] = one
            part_send[t, x] = one.astype(jnp.bfloat16)
        for d in range(1, nx):
            scatter(t, d)
        if e >= 4:
            reduce(e - 4)
    for e in range(nb - 4, nb):
        reduce(e)

    with jax.named_scope("wF"):
        await_bytes(out_ref.at[pl.ds(0, nb - 1)], f_came)

    with jax.named_scope("drain"):
        w_swap.wait_send()
        await_bytes(stage.at[pl.ds(0, m - 1)], a_sent)
        await_bytes(far, k_sent)
        await_bytes(att.at[:, pl.ds(0, side)], b_sent)

        @pl.when(is_gate)
        def _():
            await_bytes(att.at[:, pl.ds(0, side * (side - 1))], passed)

        await_bytes(part_send.at[:, pl.ds(0, nx - 1)], r_sent)
        await_bytes(final_send.at[pl.ds(0, nb - 1)], f_sent)


def fused(nb, nu, query, keys, values, out_weight, out_gain):
    nx = nu // 2
    m = nb * nx
    rows, width = query.shape
    pairs = width // LANES // m
    depth, columns = out_weight.shape
    bf16, f32 = jnp.bfloat16, jnp.float32
    vmem, dma = pltpu.VMEM, pltpu.SemaphoreType.DMA
    in_hbm = pl.BlockSpec(memory_space=pltpu.HBM)
    block = nx * rows
    gathered = pl.pallas_call(
        functools.partial(attend_kernel, nb, nu),
        out_shape=vmem((nb, rows, columns), bf16),
        in_specs=[in_hbm] * 5,
        out_specs=pl.BlockSpec(memory_space=pltpu.VMEM),
        scratch_shapes=[
            vmem((3, rows, width), bf16),
            vmem((nb, 1, columns), f32),
            vmem((m, pairs, 3, rows, LANES), bf16),
            vmem((pairs, 3, m, rows, LANES), bf16),
            vmem((pairs, 2, m, rows, LANES), bf16),
            vmem((2 * depth, columns), bf16),
            vmem((pairs, nb, nb, block, LANES), bf16),
            vmem((nb, block, columns), f32),
            vmem((nb, nx, rows, columns), f32),
            vmem((nb, nx, rows, columns), bf16),
            vmem((nb, nx, rows, columns), bf16),
            vmem((nb, rows, columns), bf16),
            dma, dma, dma, dma, dma, dma((pairs,)), dma, dma((pairs,)),
            pltpu.SemaphoreType.REGULAR((nb - 1,)),
            dma, dma((pairs, nb)), dma((nb, nb)), dma, dma, dma((nb, nx - 1)), dma, dma,
        ],
        compiler_params=pltpu.CompilerParams(
            collective_id=0, has_side_effects=True),
    )(query, keys, values, out_weight, out_gain.reshape(nb, 1, columns))
    return gathered.transpose(1, 0, 2).reshape(rows, width)


def on_any(nb, nu, query, keys, values, out_weight, out_gain):
    rows, width = query.shape
    suits = (
        nu % 2 == 0 and nu > 2 and nb % 2 == 0 and width % (LANES * nb * nu // 2) == 0
        and rows % 8 == 0 and (nu // 2 * rows) % 16 == 0 and (width // nb) % LANES == 0
    )
    plan = functools.partial(fused, nb, nu) if suits else on_device
    return plan(query, keys, values, out_weight, out_gain)


def solution(mesh):
    in_specs = (
        P(("group", "blk", "uly"), None),
        P(("group", "blk", "uly"), None),
        P(("group", "blk", "uly"), None),
        P("uly", "blk"),
        P(),
    )
    out_specs = P(("group", "blk", "uly"), None)
    body = functools.partial(on_any, mesh.shape["blk"], mesh.shape["uly"])
    return jax.shard_map(
        body, mesh=mesh, in_specs=in_specs, out_specs=out_specs, check_vma=False
    )
```

```python
import functools
import math

import jax
import jax.numpy as jnp
from jax import lax
from jax.experimental import pallas as pl
from jax.experimental.pallas import tpu as pltpu
from jax.sharding import PartitionSpec as P

HEAD = 64
LANES = 128
MESH = pl.DeviceIdType.MESH

def make_fold(query_heads, state_now, pieces):
    score_scale = 1.0 / math.sqrt(HEAD)
    head_count = query_heads.shape[1]
    running_max, denominator, weighted = state_now
    key_part, value_part = pieces
    key_count = key_part.shape[0]
    key_heads = key_part.reshape(key_count, head_count, HEAD)
    value_heads = value_part.reshape(key_count, head_count, HEAD)
    scores = (
        jnp.einsum("qhd,khd->qhk", query_heads, key_heads, preferred_element_type=jnp.float32)
        * score_scale
    )
    new_max = jnp.max(scores, axis=2)
    weights = jnp.exp(scores - new_max[:, :, None])
    shrink = jnp.exp(running_max - new_max)
    denominator = denominator * shrink + jnp.sum(weights, axis=2)
    weighted = weighted * shrink[:, :, None] + jnp.einsum(
        "qhk,khd->qhd",
        weights.astype(jnp.bfloat16),
        value_heads,
        preferred_element_type=jnp.float32,
    )
    return (new_max, denominator, weighted)


def initial_state(row_count, head_count):
    return (
        jnp.full((row_count, head_count), -jnp.inf, jnp.float32),
        jnp.zeros((row_count, head_count), jnp.float32),
        jnp.zeros((row_count, head_count, HEAD), jnp.float32),
    )


def on_device(query, keys, values, out_weight, out_gain):
    grouped_q, grouped_k, grouped_v = (
        lax.all_to_all(query, "uly", split_axis=1, concat_axis=0, tiled=True),
        lax.all_to_all(keys, "uly", split_axis=1, concat_axis=0, tiled=True),
        lax.all_to_all(values, "uly", split_axis=1, concat_axis=0, tiled=True),
    )
    row_count = grouped_q.shape[0]
    features = grouped_q.shape[1]
    local_heads = features // HEAD
    query_heads = grouped_q.reshape(row_count, local_heads, HEAD)
    half_heads = local_heads // 2
    half_width = half_heads * HEAD
    low_state = make_fold(
        query_heads[:, :half_heads],
        initial_state(row_count, half_heads),
        (
            lax.all_gather(grouped_k[:, :half_width], "blk", axis=0, tiled=True),
            lax.all_gather(grouped_v[:, :half_width], "blk", axis=0, tiled=True),
        ),
    )
    high_state = make_fold(
        query_heads[:, half_heads:],
        initial_state(row_count, local_heads - half_heads),
        (
            lax.all_gather(grouped_k[:, half_width:], "blk", axis=0, tiled=True),
            lax.all_gather(grouped_v[:, half_width:], "blk", axis=0, tiled=True),
        ),
    )
    denominator = jnp.concatenate([low_state[1], high_state[1]], axis=1)
    weighted = jnp.concatenate([low_state[2], high_state[2]], axis=1)
    attended = (
        (weighted / denominator[:, :, None]).reshape(row_count, features).astype(jnp.bfloat16)
    )
    partial_value = jnp.dot(
        attended,
        lax.all_gather(out_weight, "blk", axis=1, tiled=True),
        preferred_element_type=jnp.float32,
    )
    summed = lax.psum_scatter(
        partial_value.astype(jnp.bfloat16), "uly", scatter_dimension=0, tiled=True
    ).astype(jnp.float32)
    return (out_gain * summed).astype(jnp.bfloat16)


def attend_kernel(
    nb, nu,
    q_hbm, k_hbm, v_hbm, w_hbm, gain_hbm, out_ref,
    qkv_ref, gain_ref, stage, got, far, w_ref,
    att, acc, part_f32, part_send, part_got, final_send, direct_got,
    in_sem, w_in, w_sent, w_came, a_sent, a_came, k_sent, k_came, up_sem,
    b_sent, b_came, b_last, passed, r_sent, r_came, f_sent, f_came, d_sent, d_came,
):
    nx = nu // 2
    m = nb * nx
    rows, width = q_hbm.shape
    pairs = stage.shape[1]
    last = pairs - 1
    depth = w_hbm.shape[0]
    block = nx * rows
    mine_rows = nb * block
    side = nb // 2
    scale = math.log2(math.e) / math.sqrt(HEAD)
    me_b, me_u = lax.axis_index("blk"), lax.axis_index("uly")
    me_x, me_c = me_u // 2, lax.rem(me_u, 2)
    me = me_b * nx + me_x
    my_side = me_b // side
    gate_here = (side - 1) + my_side
    gate_there = side - my_side
    is_gate = me_b == gate_here
    held = me_b < 0
    far_side = (1 - my_side) * side

    def turn_of(b, e):
        low = nb - 1 if e == nb - 1 else (e + 1) % (nb - 1)
        upward = b // side
        return upward * e + (1 - upward) * low

    is_end = ((me_b == 0) | (me_b == nb - 1)) & (nb > 2)
    opposite = nb - 1 - me_b

    def order_here(e):
        own_last = me_b if e == nb - 1 else e + (e >= me_b)
        return is_gate * own_last + (1 - is_gate) * turn_of(me_b, e)

    def there(b, x):
        return dict(device_id={"blk": b, "uly": 2 * x + me_c}, device_id_type=MESH)

    partner = dict(device_id={"blk": me_b, "uly": 2 * me_x + 1 - me_c}, device_id_type=MESH)

    def await_bytes(ref, sem):
        pltpu.make_async_copy(ref, ref, sem).wait()

    def when(condition, action):
        pl.when(condition)(action)

    barrier = pltpu.get_barrier_semaphore()
    pl.semaphore_signal(barrier, inc=1, **partner)
    for d in range(1, nx):
        pl.semaphore_signal(barrier, inc=1, **there(me_b, lax.rem(me_x + d, nx)))
    for b in range(1, nb):

        @pl.when(b > me_b)
        def _():
            for x in range(nx):
                pl.semaphore_signal(barrier, inc=1, **there(b, x))

    for s, ref in enumerate((q_hbm, k_hbm, v_hbm)):
        pltpu.make_async_copy(ref, qkv_ref.at[s], in_sem).start()
    w_mine = w_ref.at[pl.ds(pl.multiple_of(me_c * depth, depth), depth)]
    with jax.named_scope("barrier"):
        pl.semaphore_wait(barrier, me_b * nx + nx)
    for b in range(nb - 1):

        @pl.when(b < me_b)
        def _():
            for x in range(nx):
                pl.semaphore_signal(up_sem.at[me_b - 1], inc=1, **there(b, x))

    with jax.named_scope("load"):
        await_bytes(qkv_ref, in_sem)
    w_load = pltpu.make_async_copy(w_hbm, w_mine, w_in)
    gain_load = pltpu.make_async_copy(gain_hbm, gain_ref, in_sem)
    w_load.start()
    gain_load.start()

    for b in range(nb):
        for x in range(nx):
            for p in range(pairs):
                at = ((x * nb + b) * pairs + p) * LANES
                for s in range(3):
                    stage[b * nx + x, p, s] = qkv_ref[s, :, pl.ds(at, LANES)]
    for p in range(pairs):
        for s in range(3):
            got[p, s, me] = stage[me, p, s]


    def ship(p, b, x):
        pltpu.make_async_remote_copy(
            src_ref=stage.at[b * nx + x, p], dst_ref=got.at[p, :, me],
            send_sem=a_sent, recv_sem=a_came.at[p], **there(b, x)).start()

    def ship_level(p, b):
        for d in range(nx - 1, -1, -1):
            ship(p, b, lax.rem(me_x + d, nx))

    def ship_beside(p):
        for d in range(1, nx):
            ship(p, me_b, lax.rem(me_x + d, nx))

    for p in range(pairs):
        for b in range(nb - 1):
            when(b < me_b, lambda: ship_level(p, b))
        ship_beside(p)

    w_swap = pltpu.make_async_remote_copy(
        src_ref=w_mine, dst_ref=w_mine, send_sem=w_sent, recv_sem=w_came, **partner)
    w_load.wait()
    gain_load.wait()
    w_swap.start()

    for b in range(1, nb):

        @pl.when(b > me_b)
        def _():
            with jax.named_scope(f"up{b}"):
                pl.semaphore_wait(up_sem.at[b - 1], nx)
            ship_level(0, b)
    for p in range(1, pairs):
        for b in range(nb - 1, 0, -1):
            when((b > me_b) & ((me_b > 0) | (b == 1)), lambda: ship_level(p, b))

    def swap(p):
        return pltpu.make_async_remote_copy(
            src_ref=got.at[p, pl.ds(1, 2)], dst_ref=far.at[p],
            send_sem=k_sent, recv_sem=k_came.at[p], **partner)

    def against(a, b):
        return lax.dot_general(a, b, (((1,), (1,)), ((), ())), preferred_element_type=jnp.float32)

    low = lax.broadcasted_iota(jnp.int32, (mine_rows, LANES), 1) < HEAD

    def target(d):
        return gate_there if d == 0 else my_side * side + lax.rem(me_b + d, side)

    def came(p, b, t):
        return b_came.at[p, b] if t is None else b_last.at[b, t]

    def piece(p, b, t):
        return att.at[p, b] if t is None else att.at[p, b, t]

    def push(p, d, b, t, sent, sem):
        pltpu.make_async_remote_copy(
            src_ref=piece(p, b, t), dst_ref=piece(p, b, t), send_sem=sent, recv_sem=sem,
            **there(target(d), me_x)).start()

    def spread(p, d):
        if p < last:
            push(p, d, me_b, None, b_sent, came(p, me_b, None))
        else:
            for e in range(nb):
                t = turn_of(target(d), e)
                push(p, d, me_b, t, b_sent, came(p, me_b, t))

    def spread_near(p):
        for d in range(1, side):
            spread(p, d)

    def far_of(i):
        return far_side + my_side * i + (1 - my_side) * (side - 1 - i)

    def near_of(d):
        return my_side * side + lax.rem(me_b + d, side)

    upper = my_side == 1
    late_core = (me_b < side) & (me_c == 1)

    def forward(p, turns, whose, fresh=True, only=True):
        @pl.when(is_gate & only)
        def _():
            for e in turns:
                t = turn_of(me_b, e)
                for i in whose:
                    b = far_of(i)
                    if p == last:
                        await_bytes(att.at[p, b, t], b_last.at[b, t])
                    elif fresh and e == turns[0]:
                        await_bytes(att.at[p, b], b_came.at[p, b])
                    for d in range(1, side):
                        push(p, d, b, t, passed, came(p, b, t))

    every = list(range(side))
    head, tail = range(nb - 1), range(nb - 1, nb)

    beside = [near_of(d) for d in range(side)]
    across = [far_side + i for i in range(side)]

    def weight_of(p, b):
        at = pl.multiple_of((b * pairs + p) * LANES, LANES)
        return w_ref[pl.ds(at, LANES)]

    def fill_early():
        await_bytes(w_mine, w_came)
        for p in range(last):
            for d in range(1, side):
                with jax.named_scope(f"wB{p}"):
                    await_bytes(att.at[p, beside[d]], b_came.at[p, beside[d]])
        if last:
            early = [(p, b) for p in range(last) for b in beside]
            seen = jnp.concatenate([att[p, b].reshape(mine_rows, LANES) for p, b in early], axis=1)
            weight = jnp.concatenate([weight_of(p, b) for p, b in early], axis=0)
            acc[...] = jnp.dot(seen, weight, preferred_element_type=jnp.float32).reshape(acc.shape)

    for p in range(pairs):
        with jax.named_scope(f"wA{p}"):
            await_bytes(got.at[p, :, pl.ds(0, m - 1)], a_came.at[p])
        if p == 0:
            for later in range(1, min(2, pairs)):
                for b in range(nb - 1, 1, -1):
                    when(me_b == 0, lambda: ship_level(later, b))
        swap(p).start()
        if p == last:
            for early in range(last):
                when(held, lambda: spread(early, 0))
        q_all = jnp.concatenate([got[p, 0, i].astype(jnp.float32) for i in range(m)], axis=0)
        q_two = jnp.concatenate(
            [jnp.where(low, q_all, 0.0), jnp.where(low, 0.0, q_all)], axis=0).astype(jnp.bfloat16)
        with jax.named_scope(f"wK{p}"):
            await_bytes(far.at[p], k_came.at[p])
        if p == last and last > 0:
            when(late_core, lambda: spread(last - 1, 0))
            when(jnp.logical_not(is_gate), lambda: spread_near(last - 1))
        k_all, v_all = (
            jnp.concatenate(
                [got[p, s, i].astype(jnp.float32) for i in range(m)]
                + [far[p, s - 1, i].astype(jnp.float32) for i in range(m)], axis=0
            ).astype(jnp.bfloat16)
            for s in (1, 2))
        scores = against(q_two, k_all)
        top = jnp.max(scores, axis=1, keepdims=True)
        weights = jnp.exp2((scores - top) * scale)
        total = jnp.sum(weights, axis=1, keepdims=True)
        both = jnp.dot(
            weights.astype(jnp.bfloat16), v_all, preferred_element_type=jnp.float32) / total
        joined = jnp.where(low, both[:mine_rows], both[mine_rows:]).astype(jnp.bfloat16)
        for t in range(nb):
            att[p, me_b, t] = joined[t * block:(t + 1) * block]
        with jax.named_scope(f"sB{p}"):
            if p < last:
                if p == 0:
                    for later in range(2, pairs):
                        for b in range(nb - 1, 1, -1):
                            when(me_b == 0, lambda: ship_level(later, b))
                when(jnp.logical_not(held | (late_core & (p == last - 1))), lambda: spread(p, 0))
                when(is_gate, lambda: spread_near(p))
                if p == last - 1:
                    for early in range(p):
                        when(jnp.logical_not(is_gate), lambda: spread_near(early))
                    for early, i in ():
                        with jax.named_scope(f"fa{early}{i}"):
                            forward(early, head, [i], only=upper)
            else:
                spread(p, 0)
                for early in range(last):
                    with jax.named_scope(f"fw{early}"):
                        for i in every:
                            if (early, i) in ():
                                forward(early, head, [i], only=jnp.logical_not(upper))
                            else:
                                forward(early, head, [i])
                spread_near(p)
                fill_early()
                with jax.named_scope(f"fwl"):
                    forward(last, head, every)
                for early in range(last):
                    forward(early, tail, every, fresh=False)
                with jax.named_scope(f"fwm"):
                    forward(last, tail, every)

    late = [(p, b) for p in range(pairs) for b in across] + [(last, b) for b in beside]

    def scatter(t, d):
        x = lax.rem(me_x + d, nx)
        pltpu.make_async_remote_copy(
            src_ref=part_send.at[t, x], dst_ref=part_got.at[t, me_x],
            send_sem=r_sent, recv_sem=r_came.at[t, d - 1], **there(me_b, x)).start()

    def reduce(e):
        t = order_here(e)
        total = part_f32[t, me_x]
        for d in range(1, nx):
            x = lax.rem(me_x + nx - d, nx)
            with jax.named_scope(f"wR{e}"):
                await_bytes(part_got.at[t, x], r_came.at[t, d - 1])
            total += part_got[t, x].astype(jnp.float32)
        gated = (gain_ref[me_b] * total).astype(jnp.bfloat16)

        @pl.when(me_b == t)
        def _():
            out_ref[t] = gated

        @pl.when(me_b != t)
        def _():
            final_send[t] = gated
            pltpu.make_async_remote_copy(
                src_ref=final_send.at[t], dst_ref=out_ref.at[me_b],
                send_sem=f_sent, recv_sem=f_came, **there(t, me_x)).start()

    for e in range(nb):
        t = order_here(e)
        with jax.named_scope(f"wBl{e}"):
            @pl.when(jnp.logical_not(is_gate))
            def _():
                for b in across:
                    await_bytes(att.at[:, b, t], b_last.at[b, t])

            for d in range(1, side):
                await_bytes(att.at[last, beside[d], t], b_last.at[beside[d], t])
        seen = jnp.concatenate([att[p, b, t] for p, b in late], axis=1)
        weight = jnp.concatenate([weight_of(p, b) for p, b in late], axis=0)
        part = jnp.dot(seen, weight, preferred_element_type=jnp.float32)
        if last:
            part += acc[t]
        for x in range(nx):
            one = part[x * rows:(x + 1) * rows]
            part_f32[t, x] = one
            part_send[t, x] = one.astype(jnp.bfloat16)
        straight = is_end & (t == opposite)

        @pl.when(straight)
        def _():
            for x in range(nx):
                pltpu.make_async_remote_copy(
                    src_ref=part_send.at[t, x], dst_ref=direct_got.at[me_x],
                    send_sem=d_sent, recv_sem=d_came, **there(opposite, x)).start()

        @pl.when(jnp.logical_not(straight))
        def _():
            for d in range(1, nx):
                scatter(t, d)
    for e in range(nb):
        when(jnp.logical_not(is_end & (order_here(e) == opposite)), lambda: reduce(e))

    with jax.named_scope("wF"):
        @pl.when(is_end)
        def _():
            await_bytes(direct_got, d_came)
            total = direct_got[0].astype(jnp.float32)
            for x in range(1, nx):
                total += direct_got[x].astype(jnp.float32)
            out_ref[opposite] = (gain_ref[opposite] * total).astype(jnp.bfloat16)
            if nb > 2:
                await_bytes(out_ref.at[pl.ds(0, nb - 2)], f_came)

        @pl.when(jnp.logical_not(is_end))
        def _():
            await_bytes(out_ref.at[pl.ds(0, nb - 1)], f_came)

    with jax.named_scope("drain"):
        w_swap.wait_send()
        await_bytes(stage.at[pl.ds(0, m - 1)], a_sent)
        await_bytes(far, k_sent)
        await_bytes(att.at[:, pl.ds(0, side)], b_sent)

        @pl.when(is_gate)
        def _():
            await_bytes(att.at[:, pl.ds(0, side * (side - 1))], passed)

        @pl.when(is_end)
        def _():
            await_bytes(part_send.at[0], d_sent)
            await_bytes(part_send.at[pl.ds(0, nb - 1), pl.ds(0, nx - 1)], r_sent)
            if nb > 2:
                await_bytes(final_send.at[pl.ds(0, nb - 2)], f_sent)

        @pl.when(jnp.logical_not(is_end))
        def _():
            await_bytes(part_send.at[:, pl.ds(0, nx - 1)], r_sent)
            await_bytes(final_send.at[pl.ds(0, nb - 1)], f_sent)


def fused(nb, nu, query, keys, values, out_weight, out_gain):
    nx = nu // 2
    m = nb * nx
    rows, width = query.shape
    pairs = width // LANES // m
    depth, columns = out_weight.shape
    bf16, f32 = jnp.bfloat16, jnp.float32
    vmem, dma = pltpu.VMEM, pltpu.SemaphoreType.DMA
    in_hbm = pl.BlockSpec(memory_space=pltpu.HBM)
    block = nx * rows
    gathered = pl.pallas_call(
        functools.partial(attend_kernel, nb, nu),
        out_shape=vmem((nb, rows, columns), bf16),
        in_specs=[in_hbm] * 5,
        out_specs=pl.BlockSpec(memory_space=pltpu.VMEM),
        scratch_shapes=[
            vmem((3, rows, width), bf16),
            vmem((nb, 1, columns), f32),
            vmem((m, pairs, 3, rows, LANES), bf16),
            vmem((pairs, 3, m, rows, LANES), bf16),
            vmem((pairs, 2, m, rows, LANES), bf16),
            vmem((2 * depth, columns), bf16),
            vmem((pairs, nb, nb, block, LANES), bf16),
            vmem((nb, block, columns), f32),
            vmem((nb, nx, rows, columns), f32),
            vmem((nb, nx, rows, columns), bf16),
            vmem((nb, nx, rows, columns), bf16),
            vmem((nb, rows, columns), bf16),
            vmem((nx, rows, columns), bf16),
            dma, dma, dma, dma, dma, dma((pairs,)), dma, dma((pairs,)),
            pltpu.SemaphoreType.REGULAR((nb - 1,)),
            dma, dma((pairs, nb)), dma((nb, nb)), dma, dma, dma((nb, nx - 1)), dma, dma, dma, dma,
        ],
        compiler_params=pltpu.CompilerParams(
            collective_id=0, has_side_effects=True),
    )(query, keys, values, out_weight, out_gain.reshape(nb, 1, columns))
    return gathered.transpose(1, 0, 2).reshape(rows, width)


def on_any(nb, nu, query, keys, values, out_weight, out_gain):
    rows, width = query.shape
    suits = (
        nu % 2 == 0 and nu > 2 and nb % 2 == 0 and width % (LANES * nb * nu // 2) == 0
        and rows % 8 == 0 and (nu // 2 * rows) % 16 == 0 and (width // nb) % LANES == 0
    )
    plan = functools.partial(fused, nb, nu) if suits else on_device
    return plan(query, keys, values, out_weight, out_gain)


def solution(mesh):
    in_specs = (
        P(("group", "blk", "uly"), None),
        P(("group", "blk", "uly"), None),
        P(("group", "blk", "uly"), None),
        P("uly", "blk"),
        P(),
    )
    out_specs = P(("group", "blk", "uly"), None)
    body = functools.partial(on_any, mesh.shape["blk"], mesh.shape["uly"])
    return jax.shard_map(
        body, mesh=mesh, in_specs=in_specs, out_specs=out_specs, check_vma=False
    )
```

```python
import functools
import math

import jax
import jax.numpy as jnp
from jax import lax
from jax.experimental import pallas as pl
from jax.experimental.pallas import tpu as pltpu
from jax.sharding import PartitionSpec as P

HEAD = 64
LANES = 128
MESH = pl.DeviceIdType.MESH

def make_fold(query_heads, state_now, pieces):
    score_scale = 1.0 / math.sqrt(HEAD)
    head_count = query_heads.shape[1]
    running_max, denominator, weighted = state_now
    key_part, value_part = pieces
    key_count = key_part.shape[0]
    key_heads = key_part.reshape(key_count, head_count, HEAD)
    value_heads = value_part.reshape(key_count, head_count, HEAD)
    scores = (
        jnp.einsum("qhd,khd->qhk", query_heads, key_heads, preferred_element_type=jnp.float32)
        * score_scale
    )
    new_max = jnp.max(scores, axis=2)
    weights = jnp.exp(scores - new_max[:, :, None])
    shrink = jnp.exp(running_max - new_max)
    denominator = denominator * shrink + jnp.sum(weights, axis=2)
    weighted = weighted * shrink[:, :, None] + jnp.einsum(
        "qhk,khd->qhd",
        weights.astype(jnp.bfloat16),
        value_heads,
        preferred_element_type=jnp.float32,
    )
    return (new_max, denominator, weighted)


def initial_state(row_count, head_count):
    return (
        jnp.full((row_count, head_count), -jnp.inf, jnp.float32),
        jnp.zeros((row_count, head_count), jnp.float32),
        jnp.zeros((row_count, head_count, HEAD), jnp.float32),
    )


def on_device(query, keys, values, out_weight, out_gain):
    grouped_q, grouped_k, grouped_v = (
        lax.all_to_all(query, "uly", split_axis=1, concat_axis=0, tiled=True),
        lax.all_to_all(keys, "uly", split_axis=1, concat_axis=0, tiled=True),
        lax.all_to_all(values, "uly", split_axis=1, concat_axis=0, tiled=True),
    )
    row_count = grouped_q.shape[0]
    features = grouped_q.shape[1]
    local_heads = features // HEAD
    query_heads = grouped_q.reshape(row_count, local_heads, HEAD)
    half_heads = local_heads // 2
    half_width = half_heads * HEAD
    low_state = make_fold(
        query_heads[:, :half_heads],
        initial_state(row_count, half_heads),
        (
            lax.all_gather(grouped_k[:, :half_width], "blk", axis=0, tiled=True),
            lax.all_gather(grouped_v[:, :half_width], "blk", axis=0, tiled=True),
        ),
    )
    high_state = make_fold(
        query_heads[:, half_heads:],
        initial_state(row_count, local_heads - half_heads),
        (
            lax.all_gather(grouped_k[:, half_width:], "blk", axis=0, tiled=True),
            lax.all_gather(grouped_v[:, half_width:], "blk", axis=0, tiled=True),
        ),
    )
    denominator = jnp.concatenate([low_state[1], high_state[1]], axis=1)
    weighted = jnp.concatenate([low_state[2], high_state[2]], axis=1)
    attended = (
        (weighted / denominator[:, :, None]).reshape(row_count, features).astype(jnp.bfloat16)
    )
    partial_value = jnp.dot(
        attended,
        lax.all_gather(out_weight, "blk", axis=1, tiled=True),
        preferred_element_type=jnp.float32,
    )
    summed = lax.psum_scatter(
        partial_value.astype(jnp.bfloat16), "uly", scatter_dimension=0, tiled=True
    ).astype(jnp.float32)
    return (out_gain * summed).astype(jnp.bfloat16)


def attend_kernel(
    nb, nu,
    q_hbm, k_hbm, v_hbm, w_hbm, gain_hbm, out_ref,
    qkv_ref, gain_ref, stage, got, far, w_ref,
    att, acc, part_f32, part_send, part_got, final_send, direct_got,
    in_sem, w_in, w_sent, w_came, a_sent, a_came, k_sent, k_came, up_sem,
    b_sent, b_came, b_last, passed, r_sent, r_came, f_sent, f_came, d_sent, d_came,
):
    nx = nu // 2
    m = nb * nx
    rows, width = q_hbm.shape
    pairs = stage.shape[1]
    last = pairs - 1
    depth = w_hbm.shape[0]
    block = nx * rows
    mine_rows = nb * block
    side = nb // 2
    scale = math.log2(math.e) / math.sqrt(HEAD)
    me_b, me_u = lax.axis_index("blk"), lax.axis_index("uly")
    me_x, me_c = me_u // 2, lax.rem(me_u, 2)
    me = me_b * nx + me_x
    my_side = me_b // side
    gate_here = (side - 1) + my_side
    gate_there = side - my_side
    is_gate = me_b == gate_here
    held = (me_b < side) & jnp.logical_not(is_gate) & (lax.rem(me_u, 2) == 1)
    far_side = (1 - my_side) * side

    def turn_of(b, e):
        low = nb - 1 if e == nb - 1 else (e + 1) % (nb - 1)
        upward = b // side
        return upward * e + (1 - upward) * low

    is_end = ((me_b == 0) | (me_b == nb - 1)) & (nb > 2)
    opposite = nb - 1 - me_b

    def order_here(e):
        own_last = me_b if e == nb - 1 else e + (e >= me_b)
        return is_gate * own_last + (1 - is_gate) * turn_of(me_b, e)

    def there(b, x):
        return dict(device_id={"blk": b, "uly": 2 * x + me_c}, device_id_type=MESH)

    partner = dict(device_id={"blk": me_b, "uly": 2 * me_x + 1 - me_c}, device_id_type=MESH)

    def await_bytes(ref, sem):
        pltpu.make_async_copy(ref, ref, sem).wait()

    def when(condition, action):
        pl.when(condition)(action)

    barrier = pltpu.get_barrier_semaphore()
    pl.semaphore_signal(barrier, inc=1, **partner)
    for d in range(1, nx):
        pl.semaphore_signal(barrier, inc=1, **there(me_b, lax.rem(me_x + d, nx)))
    for b in range(1, nb):

        @pl.when(b > me_b)
        def _():
            for x in range(nx):
                pl.semaphore_signal(barrier, inc=1, **there(b, x))

    for s, ref in enumerate((q_hbm, k_hbm, v_hbm)):
        pltpu.make_async_copy(ref, qkv_ref.at[s], in_sem).start()
    w_mine = w_ref.at[pl.ds(pl.multiple_of(me_c * depth, depth), depth)]
    with jax.named_scope("barrier"):
        pl.semaphore_wait(barrier, me_b * nx + nx)
    for b in range(nb - 1):

        @pl.when(b < me_b)
        def _():
            for x in range(nx):
                pl.semaphore_signal(up_sem.at[me_b - 1], inc=1, **there(b, x))

    with jax.named_scope("load"):
        await_bytes(qkv_ref, in_sem)
    w_load = pltpu.make_async_copy(w_hbm, w_mine, w_in)
    gain_load = pltpu.make_async_copy(gain_hbm, gain_ref, in_sem)
    w_load.start()
    gain_load.start()

    for b in range(nb):
        for x in range(nx):
            for p in range(pairs):
                at = ((x * nb + b) * pairs + p) * LANES
                for s in range(3):
                    stage[b * nx + x, p, s] = qkv_ref[s, :, pl.ds(at, LANES)]
    for p in range(pairs):
        for s in range(3):
            got[p, s, me] = stage[me, p, s]


    def ship(p, b, x):
        pltpu.make_async_remote_copy(
            src_ref=stage.at[b * nx + x, p], dst_ref=got.at[p, :, me],
            send_sem=a_sent, recv_sem=a_came.at[p], **there(b, x)).start()

    def ship_level(p, b):
        for d in range(nx - 1, -1, -1):
            ship(p, b, lax.rem(me_x + d, nx))

    def ship_beside(p):
        for d in range(1, nx):
            ship(p, me_b, lax.rem(me_x + d, nx))

    for p in range(pairs):
        for b in range(nb - 1):
            when(b < me_b, lambda: ship_level(p, b))
        ship_beside(p)

    w_swap = pltpu.make_async_remote_copy(
        src_ref=w_mine, dst_ref=w_mine, send_sem=w_sent, recv_sem=w_came, **partner)
    w_load.wait()
    gain_load.wait()
    w_swap.start()

    for b in range(1, nb):

        @pl.when(b > me_b)
        def _():
            with jax.named_scope(f"up{b}"):
                pl.semaphore_wait(up_sem.at[b - 1], nx)
            ship_level(0, b)
    for p in range(1, pairs):
        for b in range(nb - 1, 0, -1):
            when((b > me_b) & ((me_b > 0) | (b == 1)), lambda: ship_level(p, b))

    def swap(p):
        return pltpu.make_async_remote_copy(
            src_ref=got.at[p, pl.ds(1, 2)], dst_ref=far.at[p],
            send_sem=k_sent, recv_sem=k_came.at[p], **partner)

    def against(a, b):
        return lax.dot_general(a, b, (((1,), (1,)), ((), ())), preferred_element_type=jnp.float32)

    low = lax.broadcasted_iota(jnp.int32, (mine_rows, LANES), 1) < HEAD

    def target(d):
        return gate_there if d == 0 else my_side * side + lax.rem(me_b + d, side)

    def came(p, b, t):
        return b_came.at[p, b] if t is None else b_last.at[b, t]

    def piece(p, b, t):
        return att.at[p, b] if t is None else att.at[p, b, t]

    def push(p, d, b, t, sent, sem):
        pltpu.make_async_remote_copy(
            src_ref=piece(p, b, t), dst_ref=piece(p, b, t), send_sem=sent, recv_sem=sem,
            **there(target(d), me_x)).start()

    def spread(p, d):
        if p < last:
            push(p, d, me_b, None, b_sent, came(p, me_b, None))
        else:
            for e in range(nb):
                t = turn_of(target(d), e)
                push(p, d, me_b, t, b_sent, came(p, me_b, t))

    def spread_near(p):
        for d in range(1, side):
            spread(p, d)

    def spread_near_turn(e):
        for d in range(1, side):
            t = turn_of(target(d), e)
            push(last, d, me_b, t, b_sent, came(last, me_b, t))

    def near_rest():
        for e in range(1, nb):
            spread_near_turn(e)

    columns = w_hbm.shape[1]

    def column(b):
        return out_ref.at[:, pl.ds(pl.multiple_of(b * columns, LANES), columns)]

    def far_of(i):
        return far_side + my_side * i + (1 - my_side) * (side - 1 - i)

    def near_of(d):
        return my_side * side + lax.rem(me_b + d, side)

    upper = my_side == 1
    late_core = is_gate & (me_c == 1)

    def forward(p, turns, whose, fresh=True, only=True):
        @pl.when(is_gate & only)
        def _():
            for e in turns:
                t = turn_of(me_b, e)
                for i in whose:
                    b = far_of(i)
                    if p == last:
                        await_bytes(att.at[p, b, t], b_last.at[b, t])
                    elif fresh and e == turns[0]:
                        await_bytes(att.at[p, b], b_came.at[p, b])
                    for d in range(1, side):
                        push(p, d, b, t, passed, came(p, b, t))

    every = list(range(side))
    head, tail = range(nb - 1), range(nb - 1, nb)

    beside = [near_of(d) for d in range(side)]
    across = [far_side + i for i in range(side)]

    def weight_of(p, b):
        at = pl.multiple_of((b * pairs + p) * LANES, LANES)
        return w_ref[pl.ds(at, LANES)]

    def fill_early():
        await_bytes(w_mine, w_came)
        for p in range(last):
            for d in range(1, side):
                with jax.named_scope(f"wB{p}"):
                    await_bytes(att.at[p, beside[d]], b_came.at[p, beside[d]])
        if last:
            early = [(p, b) for p in range(last) for b in beside]
            seen = jnp.concatenate([att[p, b].reshape(mine_rows, LANES) for p, b in early], axis=1)
            weight = jnp.concatenate([weight_of(p, b) for p, b in early], axis=0)
            acc[...] = jnp.dot(seen, weight, preferred_element_type=jnp.float32).reshape(acc.shape)

    for p in range(pairs):
        with jax.named_scope(f"wA{p}"):
            await_bytes(got.at[p, :, pl.ds(0, m - 1)], a_came.at[p])
        if p == 0:
            for later in range(1, min(2, pairs)):
                for b in range(nb - 1, 1, -1):
                    when(me_b == 0, lambda: ship_level(later, b))
        swap(p).start()
        if p == last:
            for early in range(last):
                when(held, lambda: spread(early, 0))
        q_all = jnp.concatenate([got[p, 0, i].astype(jnp.float32) for i in range(m)], axis=0)
        q_two = jnp.concatenate(
            [jnp.where(low, q_all, 0.0), jnp.where(low, 0.0, q_all)], axis=0).astype(jnp.bfloat16)
        with jax.named_scope(f"wK{p}"):
            await_bytes(far.at[p], k_came.at[p])
        if p == last and last > 0:
            when(late_core, lambda: spread(last - 1, 0))
            when(jnp.logical_not(is_gate), lambda: spread_near(last - 1))
        k_all, v_all = (
            jnp.concatenate(
                [got[p, s, i].astype(jnp.float32) for i in range(m)]
                + [far[p, s - 1, i].astype(jnp.float32) for i in range(m)], axis=0
            ).astype(jnp.bfloat16)
            for s in (1, 2))
        scores = against(q_two, k_all)
        top = jnp.max(scores, axis=1, keepdims=True)
        weights = jnp.exp2((scores - top) * scale)
        total = jnp.sum(weights, axis=1, keepdims=True)
        both = jnp.dot(
            weights.astype(jnp.bfloat16), v_all, preferred_element_type=jnp.float32) / total
        joined = jnp.where(low, both[:mine_rows], both[mine_rows:]).astype(jnp.bfloat16)
        for t in range(nb):
            att[p, me_b, t] = joined[t * block:(t + 1) * block]
        with jax.named_scope(f"sB{p}"):
            if p < last:
                if p == 0:
                    for later in range(2, pairs):
                        for b in range(nb - 1, 1, -1):
                            when(me_b == 0, lambda: ship_level(later, b))
                when(jnp.logical_not(held | (late_core & (p == last - 1))), lambda: spread(p, 0))
                when(is_gate, lambda: spread_near(p))
                if p == last - 1:
                    for early in range(p):
                        when(jnp.logical_not(is_gate), lambda: spread_near(early))
                    for early, i in ():
                        with jax.named_scope(f"fa{early}{i}"):
                            forward(early, head, [i], only=upper)
            else:
                spread(p, 0)
                for early in range(last):
                    with jax.named_scope(f"fw{early}"):
                        for i in every:
                            if (early, i) in ():
                                forward(early, head, [i], only=jnp.logical_not(upper))
                            else:
                                forward(early, head, [i])
                spread_near_turn(0)
                when(my_side == 0, near_rest)
                fill_early()
                with jax.named_scope("fwl"):
                    forward(last, head[:1], every)
                when(my_side == 1, near_rest)
                with jax.named_scope("fwk"):
                    forward(last, head[1:], every)
                for early in range(last):
                    forward(early, tail, every, fresh=False)
                with jax.named_scope(f"fwm"):
                    forward(last, tail, every)

    late = [(p, b) for p in range(pairs) for b in across] + [(last, b) for b in beside]

    def scatter(t, d):
        x = lax.rem(me_x + d, nx)
        pltpu.make_async_remote_copy(
            src_ref=part_send.at[t, x], dst_ref=part_got.at[t, me_x],
            send_sem=r_sent, recv_sem=r_came.at[t, d - 1], **there(me_b, x)).start()

    def reduce(e):
        t = order_here(e)
        total = part_f32[t, me_x]
        for d in range(1, nx):
            x = lax.rem(me_x + nx - d, nx)
            with jax.named_scope(f"wR{e}"):
                await_bytes(part_got.at[t, x], r_came.at[t, d - 1])
            total += part_got[t, x].astype(jnp.float32)
        gated = (gain_ref[me_b] * total).astype(jnp.bfloat16)

        @pl.when(me_b == t)
        def _():
            out_ref[:, pl.ds(pl.multiple_of(t * columns, LANES), columns)] = gated

        @pl.when(me_b != t)
        def _():
            final_send[t] = gated
            pltpu.make_async_remote_copy(
                src_ref=final_send.at[t], dst_ref=column(me_b),
                send_sem=f_sent, recv_sem=f_came, **there(t, me_x)).start()

    for e in range(nb):
        t = order_here(e)
        with jax.named_scope(f"wBl{e}"):
            @pl.when(jnp.logical_not(is_gate))
            def _():
                for b in across:
                    await_bytes(att.at[:, b, t], b_last.at[b, t])

            for d in range(1, side):
                await_bytes(att.at[last, beside[d], t], b_last.at[beside[d], t])
        seen = jnp.concatenate([att[p, b, t] for p, b in late], axis=1)
        weight = jnp.concatenate([weight_of(p, b) for p, b in late], axis=0)
        part = jnp.dot(seen, weight, preferred_element_type=jnp.float32)
        if last:
            part += acc[t]
        for x in range(nx):
            one = part[x * rows:(x + 1) * rows]
            part_f32[t, x] = one
            part_send[t, x] = one.astype(jnp.bfloat16)
        straight = is_end & (t == opposite)

        @pl.when(straight)
        def _():
            for x in range(nx):
                pltpu.make_async_remote_copy(
                    src_ref=part_send.at[t, x], dst_ref=direct_got.at[me_x],
                    send_sem=d_sent, recv_sem=d_came, **there(opposite, x)).start()

        @pl.when(jnp.logical_not(straight))
        def _():
            for d in range(1, nx):
                scatter(t, d)
    for e in range(nb):
        when(jnp.logical_not(is_end & (order_here(e) == opposite)), lambda: reduce(e))

    with jax.named_scope("wF"):
        @pl.when(is_end)
        def _():
            await_bytes(direct_got, d_came)
            total = direct_got[0].astype(jnp.float32)
            for x in range(1, nx):
                total += direct_got[x].astype(jnp.float32)
            out_ref[:, pl.ds(pl.multiple_of(opposite * columns, LANES), columns)] = (
                gain_ref[opposite] * total).astype(jnp.bfloat16)
            if nb > 2:
                await_bytes(out_ref.at[:, pl.ds(0, (nb - 2) * columns)], f_came)

        @pl.when(jnp.logical_not(is_end))
        def _():
            await_bytes(out_ref.at[:, pl.ds(0, (nb - 1) * columns)], f_came)

    with jax.named_scope("drain"):
        w_swap.wait_send()
        await_bytes(stage.at[pl.ds(0, m - 1)], a_sent)
        await_bytes(far, k_sent)
        await_bytes(att.at[:, pl.ds(0, side)], b_sent)

        @pl.when(is_gate)
        def _():
            await_bytes(att.at[:, pl.ds(0, side * (side - 1))], passed)

        @pl.when(is_end)
        def _():
            await_bytes(part_send.at[0], d_sent)
            await_bytes(part_send.at[pl.ds(0, nb - 1), pl.ds(0, nx - 1)], r_sent)
            if nb > 2:
                await_bytes(final_send.at[pl.ds(0, nb - 2)], f_sent)

        @pl.when(jnp.logical_not(is_end))
        def _():
            await_bytes(part_send.at[:, pl.ds(0, nx - 1)], r_sent)
            await_bytes(final_send.at[pl.ds(0, nb - 1)], f_sent)


def fused(nb, nu, query, keys, values, out_weight, out_gain):
    nx = nu // 2
    m = nb * nx
    rows, width = query.shape
    pairs = width // LANES // m
    depth, columns = out_weight.shape
    bf16, f32 = jnp.bfloat16, jnp.float32
    vmem, dma = pltpu.VMEM, pltpu.SemaphoreType.DMA
    in_hbm = pl.BlockSpec(memory_space=pltpu.HBM)
    block = nx * rows
    gathered = pl.pallas_call(
        functools.partial(attend_kernel, nb, nu),
        out_shape=vmem((rows, nb * columns), bf16),
        in_specs=[in_hbm] * 5,
        out_specs=pl.BlockSpec(memory_space=pltpu.VMEM),
        scratch_shapes=[
            vmem((3, rows, width), bf16),
            vmem((nb, 1, columns), f32),
            vmem((m, pairs, 3, rows, LANES), bf16),
            vmem((pairs, 3, m, rows, LANES), bf16),
            vmem((pairs, 2, m, rows, LANES), bf16),
            vmem((2 * depth, columns), bf16),
            vmem((pairs, nb, nb, block, LANES), bf16),
            vmem((nb, block, columns), f32),
            vmem((nb, nx, rows, columns), f32),
            vmem((nb, nx, rows, columns), bf16),
            vmem((nb, nx, rows, columns), bf16),
            vmem((nb, rows, columns), bf16),
            vmem((nx, rows, columns), bf16),
            dma, dma, dma, dma, dma, dma((pairs,)), dma, dma((pairs,)),
            pltpu.SemaphoreType.REGULAR((nb - 1,)),
            dma, dma((pairs, nb)), dma((nb, nb)), dma, dma, dma((nb, nx - 1)), dma, dma, dma, dma,
        ],
        compiler_params=pltpu.CompilerParams(
            collective_id=0, has_side_effects=True),
    )(query, keys, values, out_weight, out_gain.reshape(nb, 1, columns))
    return gathered


def on_any(nb, nu, query, keys, values, out_weight, out_gain):
    rows, width = query.shape
    suits = (
        nu % 2 == 0 and nu > 2 and nb % 2 == 0 and width % (LANES * nb * nu // 2) == 0
        and rows % 8 == 0 and (nu // 2 * rows) % 16 == 0 and (width // nb) % LANES == 0
    )
    plan = functools.partial(fused, nb, nu) if suits else on_device
    return plan(query, keys, values, out_weight, out_gain)


def solution(mesh):
    in_specs = (
        P(("group", "blk", "uly"), None),
        P(("group", "blk", "uly"), None),
        P(("group", "blk", "uly"), None),
        P("uly", "blk"),
        P(),
    )
    out_specs = P(("group", "blk", "uly"), None)
    body = functools.partial(on_any, mesh.shape["blk"], mesh.shape["uly"])
    return jax.shard_map(
        body, mesh=mesh, in_specs=in_specs, out_specs=out_specs, check_vma=False
    )
```

```python
import functools
import math

import jax
import jax.numpy as jnp
from jax import lax
from jax.experimental import pallas as pl
from jax.experimental.pallas import tpu as pltpu
from jax.sharding import PartitionSpec as P

HEAD = 64
LANES = 128
MESH = pl.DeviceIdType.MESH

def make_fold(query_heads, state_now, pieces):
    score_scale = 1.0 / math.sqrt(HEAD)
    head_count = query_heads.shape[1]
    running_max, denominator, weighted = state_now
    key_part, value_part = pieces
    key_count = key_part.shape[0]
    key_heads = key_part.reshape(key_count, head_count, HEAD)
    value_heads = value_part.reshape(key_count, head_count, HEAD)
    scores = (
        jnp.einsum("qhd,khd->qhk", query_heads, key_heads, preferred_element_type=jnp.float32)
        * score_scale
    )
    new_max = jnp.max(scores, axis=2)
    weights = jnp.exp(scores - new_max[:, :, None])
    shrink = jnp.exp(running_max - new_max)
    denominator = denominator * shrink + jnp.sum(weights, axis=2)
    weighted = weighted * shrink[:, :, None] + jnp.einsum(
        "qhk,khd->qhd",
        weights.astype(jnp.bfloat16),
        value_heads,
        preferred_element_type=jnp.float32,
    )
    return (new_max, denominator, weighted)


def initial_state(row_count, head_count):
    return (
        jnp.full((row_count, head_count), -jnp.inf, jnp.float32),
        jnp.zeros((row_count, head_count), jnp.float32),
        jnp.zeros((row_count, head_count, HEAD), jnp.float32),
    )


def on_device(query, keys, values, out_weight, out_gain):
    grouped_q, grouped_k, grouped_v = (
        lax.all_to_all(query, "uly", split_axis=1, concat_axis=0, tiled=True),
        lax.all_to_all(keys, "uly", split_axis=1, concat_axis=0, tiled=True),
        lax.all_to_all(values, "uly", split_axis=1, concat_axis=0, tiled=True),
    )
    row_count = grouped_q.shape[0]
    features = grouped_q.shape[1]
    local_heads = features // HEAD
    query_heads = grouped_q.reshape(row_count, local_heads, HEAD)
    half_heads = local_heads // 2
    half_width = half_heads * HEAD
    low_state = make_fold(
        query_heads[:, :half_heads],
        initial_state(row_count, half_heads),
        (
            lax.all_gather(grouped_k[:, :half_width], "blk", axis=0, tiled=True),
            lax.all_gather(grouped_v[:, :half_width], "blk", axis=0, tiled=True),
        ),
    )
    high_state = make_fold(
        query_heads[:, half_heads:],
        initial_state(row_count, local_heads - half_heads),
        (
            lax.all_gather(grouped_k[:, half_width:], "blk", axis=0, tiled=True),
            lax.all_gather(grouped_v[:, half_width:], "blk", axis=0, tiled=True),
        ),
    )
    denominator = jnp.concatenate([low_state[1], high_state[1]], axis=1)
    weighted = jnp.concatenate([low_state[2], high_state[2]], axis=1)
    attended = (
        (weighted / denominator[:, :, None]).reshape(row_count, features).astype(jnp.bfloat16)
    )
    partial_value = jnp.dot(
        attended,
        lax.all_gather(out_weight, "blk", axis=1, tiled=True),
        preferred_element_type=jnp.float32,
    )
    summed = lax.psum_scatter(
        partial_value.astype(jnp.bfloat16), "uly", scatter_dimension=0, tiled=True
    ).astype(jnp.float32)
    return (out_gain * summed).astype(jnp.bfloat16)


def attend_kernel(
    nb, nu,
    q_hbm, k_hbm, v_hbm, w_hbm, gain_hbm, out_ref,
    qkv_ref, gain_ref, stage, got, far, w_ref,
    att, acc, part_f32, part_send, part_got, final_send, direct_got,
    in_sem, w_in, w_sent, w_came, a_sent, a_came, k_sent, k_came, up_sem,
    b_sent, b_came, b_last, passed, r_sent, r_came, f_sent, f_came, d_sent, d_came,
):
    nx = nu // 2
    m = nb * nx
    rows, width = q_hbm.shape
    pairs = stage.shape[1]
    last = pairs - 1
    depth = w_hbm.shape[0]
    block = nx * rows
    mine_rows = nb * block
    side = nb // 2
    scale = math.log2(math.e) / math.sqrt(HEAD)
    me_b, me_u = lax.axis_index("blk"), lax.axis_index("uly")
    me_x, me_c = me_u // 2, lax.rem(me_u, 2)
    me = me_b * nx + me_x
    my_side = me_b // side
    gate_here = (side - 1) + my_side
    gate_there = side - my_side
    is_gate = me_b == gate_here
    held = (me_b < side) & jnp.logical_not(is_gate) & (lax.rem(me_u, 2) == 1)
    far_side = (1 - my_side) * side

    def turn_of(b, e):
        low = nb - 1 if e == nb - 1 else (e + 1) % (nb - 1)
        upward = b // side
        return upward * e + (1 - upward) * low

    is_end = ((me_b == 0) | (me_b == nb - 1)) & (nb > 2)
    opposite = nb - 1 - me_b

    def order_here(e):
        own_last = me_b if e == nb - 1 else e + (e >= me_b)
        return is_gate * own_last + (1 - is_gate) * turn_of(me_b, e)

    def there(b, x):
        return dict(device_id={"blk": b, "uly": 2 * x + me_c}, device_id_type=MESH)

    partner = dict(device_id={"blk": me_b, "uly": 2 * me_x + 1 - me_c}, device_id_type=MESH)

    def await_bytes(ref, sem):
        pltpu.make_async_copy(ref, ref, sem).wait()

    def when(condition, action):
        pl.when(condition)(action)

    barrier = pltpu.get_barrier_semaphore()
    pl.semaphore_signal(barrier, inc=1, **partner)
    for d in range(1, nx):
        pl.semaphore_signal(barrier, inc=1, **there(me_b, lax.rem(me_x + d, nx)))
    for b in range(1, nb):

        @pl.when(b > me_b)
        def _():
            for x in range(nx):
                pl.semaphore_signal(barrier, inc=1, **there(b, x))

    for s, ref in enumerate((q_hbm, k_hbm, v_hbm)):
        pltpu.make_async_copy(ref, qkv_ref.at[s], in_sem).start()
    w_mine = w_ref.at[pl.ds(pl.multiple_of(me_c * depth, depth), depth)]
    with jax.named_scope("barrier"):
        pl.semaphore_wait(barrier, me_b * nx + nx)
    for b in range(nb - 1):

        @pl.when(b < me_b)
        def _():
            for x in range(nx):
                pl.semaphore_signal(up_sem.at[me_b - 1], inc=1, **there(b, x))

    with jax.named_scope("load"):
        await_bytes(qkv_ref, in_sem)
    w_load = pltpu.make_async_copy(w_hbm, w_mine, w_in)
    gain_load = pltpu.make_async_copy(gain_hbm, gain_ref, in_sem)
    w_load.start()
    gain_load.start()

    for b in range(nb):
        for x in range(nx):
            for p in range(pairs):
                at = ((x * nb + b) * pairs + p) * LANES
                for s in range(3):
                    stage[b * nx + x, p, s] = qkv_ref[s, :, pl.ds(at, LANES)]
    for p in range(pairs):
        for s in range(3):
            got[p, s, me] = stage[me, p, s]


    def ship(p, b, x):
        pltpu.make_async_remote_copy(
            src_ref=stage.at[b * nx + x, p], dst_ref=got.at[p, :, me],
            send_sem=a_sent, recv_sem=a_came.at[p], **there(b, x)).start()

    def ship_level(p, b):
        for d in range(nx - 1, -1, -1):
            ship(p, b, lax.rem(me_x + d, nx))

    def ship_beside(p):
        for d in range(1, nx):
            ship(p, me_b, lax.rem(me_x + d, nx))

    for p in range(pairs):
        for b in range(nb - 1):
            when(b < me_b, lambda: ship_level(p, b))
        ship_beside(p)

    w_swap = pltpu.make_async_remote_copy(
        src_ref=w_mine, dst_ref=w_mine, send_sem=w_sent, recv_sem=w_came, **partner)
    w_load.wait()
    gain_load.wait()
    w_swap.start()

    for b in range(1, nb):

        @pl.when(b > me_b)
        def _():
            with jax.named_scope(f"up{b}"):
                pl.semaphore_wait(up_sem.at[b - 1], nx)
            ship_level(0, b)
    for p in range(1, pairs):
        for b in range(nb - 1, 0, -1):
            when((b > me_b) & ((me_b > 0) | (b == 1)), lambda: ship_level(p, b))

    def swap(p):
        return pltpu.make_async_remote_copy(
            src_ref=got.at[p, pl.ds(1, 2)], dst_ref=far.at[p],
            send_sem=k_sent, recv_sem=k_came.at[p], **partner)

    def against(a, b):
        return lax.dot_general(a, b, (((1,), (1,)), ((), ())), preferred_element_type=jnp.float32)

    low = lax.broadcasted_iota(jnp.int32, (mine_rows, LANES), 1) < HEAD

    def target(d):
        return gate_there if d == 0 else my_side * side + lax.rem(me_b + d, side)

    def came(p, b, t, taker):
        slot = b - (b > taker)
        return b_came.at[p, slot] if t is None else b_last.at[slot, t]

    def piece(p, b, t):
        return att.at[p, b] if t is None else att.at[p, b, t]

    def push(p, d, b, t, sent, sem):
        pltpu.make_async_remote_copy(
            src_ref=piece(p, b, t), dst_ref=piece(p, b, t), send_sem=sent, recv_sem=sem,
            **there(target(d), me_x)).start()

    def spread(p, d):
        if p < last:
            push(p, d, me_b, None, b_sent, came(p, me_b, None, target(d)))
        else:
            for e in range(nb):
                t = turn_of(target(d), e)
                push(p, d, me_b, t, b_sent, came(p, me_b, t, target(d)))

    def spread_near(p):
        for d in range(1, side):
            spread(p, d)

    def spread_near_turn(e):
        for d in range(1, side):
            t = turn_of(target(d), e)
            push(last, d, me_b, t, b_sent, came(last, me_b, t, target(d)))

    def near_rest():
        for e in range(1, nb):
            spread_near_turn(e)

    columns = w_hbm.shape[1]

    def column(b):
        return out_ref.at[:, pl.ds(pl.multiple_of(b * columns, LANES), columns)]

    def far_of(i):
        return far_side + my_side * i + (1 - my_side) * (side - 1 - i)

    def near_of(d):
        return my_side * side + lax.rem(me_b + d, side)

    upper = my_side == 1
    late_core = is_gate & (me_c == 1)

    def forward(p, turns, whose, fresh=True, only=True):
        @pl.when(is_gate & only)
        def _():
            for e in turns:
                t = turn_of(me_b, e)
                for i in whose:
                    b = far_of(i)
                    if p == last:
                        await_bytes(att.at[p, b, t], came(last, b, t, me_b))
                    elif fresh and e == turns[0]:
                        await_bytes(att.at[p, b], came(p, b, None, me_b))
                    for d in range(1, side):
                        push(p, d, b, t, passed, came(p, b, t, target(d)))

    every = list(range(side))
    head, tail = range(nb - 1), range(nb - 1, nb)

    beside = [near_of(d) for d in range(side)]
    across = [far_side + i for i in range(side)]

    def weight_of(p, b):
        at = pl.multiple_of((b * pairs + p) * LANES, LANES)
        return w_ref[pl.ds(at, LANES)]

    def fill_early():
        await_bytes(w_mine, w_came)
        for p in range(last):
            for d in range(1, side):
                with jax.named_scope(f"wB{p}"):
                    await_bytes(att.at[p, beside[d]], came(p, beside[d], None, me_b))
        if last:
            early = [(p, b) for p in range(last) for b in beside]
            seen = jnp.concatenate([att[p, b].reshape(mine_rows, LANES) for p, b in early], axis=1)
            weight = jnp.concatenate([weight_of(p, b) for p, b in early], axis=0)
            acc[...] = jnp.dot(seen, weight, preferred_element_type=jnp.float32).reshape(acc.shape)

    for p in range(pairs):
        with jax.named_scope(f"wA{p}"):
            await_bytes(got.at[p, :, pl.ds(0, m - 1)], a_came.at[p])
        if p == 0:
            for later in range(1, min(2, pairs)):
                for b in range(nb - 1, 1, -1):
                    when(me_b == 0, lambda: ship_level(later, b))
        swap(p).start()
        if p == last:
            for early in range(last):
                when(held, lambda: spread(early, 0))
        q_all = jnp.concatenate([got[p, 0, i].astype(jnp.float32) for i in range(m)], axis=0)
        q_two = jnp.concatenate(
            [jnp.where(low, q_all, 0.0), jnp.where(low, 0.0, q_all)], axis=0).astype(jnp.bfloat16)
        with jax.named_scope(f"wK{p}"):
            await_bytes(far.at[p], k_came.at[p])
        if p == last and last > 0:
            when(late_core, lambda: spread(last - 1, 0))
            when(jnp.logical_not(is_gate), lambda: spread_near(last - 1))
        k_all, v_all = (
            jnp.concatenate(
                [got[p, s, i].astype(jnp.float32) for i in range(m)]
                + [far[p, s - 1, i].astype(jnp.float32) for i in range(m)], axis=0
            ).astype(jnp.bfloat16)
            for s in (1, 2))
        scores = against(q_two, k_all)
        top = jnp.max(scores, axis=1, keepdims=True)
        weights = jnp.exp2((scores - top) * scale)
        total = jnp.sum(weights, axis=1, keepdims=True)
        both = jnp.dot(
            weights.astype(jnp.bfloat16), v_all, preferred_element_type=jnp.float32) / total
        joined = jnp.where(low, both[:mine_rows], both[mine_rows:]).astype(jnp.bfloat16)
        for t in range(nb):
            att[p, me_b, t] = joined[t * block:(t + 1) * block]
        with jax.named_scope(f"sB{p}"):
            if p < last:
                if p == 0:
                    for later in range(2, pairs):
                        for b in range(nb - 1, 1, -1):
                            when(me_b == 0, lambda: ship_level(later, b))
                when(jnp.logical_not(held | (late_core & (p == last - 1))), lambda: spread(p, 0))
                when(is_gate, lambda: spread_near(p))
                if p == last - 1:
                    for early in range(p):
                        when(jnp.logical_not(is_gate), lambda: spread_near(early))
                    for early, i in ():
                        with jax.named_scope(f"fa{early}{i}"):
                            forward(early, head, [i], only=upper)
            else:
                spread(p, 0)
                for early in range(last):
                    with jax.named_scope(f"fw{early}"):
                        for i in every:
                            if (early, i) in ():
                                forward(early, head, [i], only=jnp.logical_not(upper))
                            else:
                                forward(early, head, [i])
                spread_near_turn(0)
                when(my_side == 0, near_rest)
                fill_early()
                with jax.named_scope("fwl"):
                    forward(last, head[:1], every)
                when(my_side == 1, near_rest)
                with jax.named_scope("fwk"):
                    forward(last, head[1:], every)
                for early in range(last):
                    forward(early, tail, every, fresh=False)
                with jax.named_scope(f"fwm"):
                    forward(last, tail, every)

    late = [(p, b) for p in range(pairs) for b in across] + [(last, b) for b in beside]

    def scatter(t, d):
        x = lax.rem(me_x + d, nx)
        pltpu.make_async_remote_copy(
            src_ref=part_send.at[t, x], dst_ref=part_got.at[t, me_x],
            send_sem=r_sent, recv_sem=r_came.at[t, d - 1], **there(me_b, x)).start()

    def reduce(e):
        t = order_here(e)
        total = part_f32[t, me_x]
        for d in range(1, nx):
            x = lax.rem(me_x + nx - d, nx)
            with jax.named_scope(f"wR{e}"):
                await_bytes(part_got.at[t, x], r_came.at[t, d - 1])
            total += part_got[t, x].astype(jnp.float32)
        gated = (gain_ref[me_b] * total).astype(jnp.bfloat16)

        @pl.when(me_b == t)
        def _():
            out_ref[:, pl.ds(pl.multiple_of(t * columns, LANES), columns)] = gated

        @pl.when(me_b != t)
        def _():
            final_send[t] = gated
            pltpu.make_async_remote_copy(
                src_ref=final_send.at[t], dst_ref=column(me_b),
                send_sem=f_sent, recv_sem=f_came, **there(t, me_x)).start()

    for e in range(nb):
        t = order_here(e)
        with jax.named_scope(f"wBl{e}"):
            @pl.when(jnp.logical_not(is_gate))
            def _():
                for b in across:
                    await_bytes(att.at[:, b, t], came(last, b, t, me_b))

            for d in range(1, side):
                await_bytes(att.at[last, beside[d], t], came(last, beside[d], t, me_b))
        seen = jnp.concatenate([att[p, b, t] for p, b in late], axis=1)
        weight = jnp.concatenate([weight_of(p, b) for p, b in late], axis=0)
        part = jnp.dot(seen, weight, preferred_element_type=jnp.float32)
        if last:
            part += acc[t]
        for x in range(nx):
            one = part[x * rows:(x + 1) * rows]
            part_f32[t, x] = one
            part_send[t, x] = one.astype(jnp.bfloat16)
        straight = is_end & (t == opposite)

        @pl.when(straight)
        def _():
            for x in range(nx):
                pltpu.make_async_remote_copy(
                    src_ref=part_send.at[t, x], dst_ref=direct_got.at[me_x],
                    send_sem=d_sent, recv_sem=d_came, **there(opposite, x)).start()

        @pl.when(jnp.logical_not(straight))
        def _():
            for d in range(1, nx):
                scatter(t, d)
    for e in range(nb):
        when(jnp.logical_not(is_end & (order_here(e) == opposite)), lambda: reduce(e))

    with jax.named_scope("wF"):
        @pl.when(is_end)
        def _():
            await_bytes(direct_got, d_came)
            total = direct_got[0].astype(jnp.float32)
            for x in range(1, nx):
                total += direct_got[x].astype(jnp.float32)
            out_ref[:, pl.ds(pl.multiple_of(opposite * columns, LANES), columns)] = (
                gain_ref[opposite] * total).astype(jnp.bfloat16)
            if nb > 2:
                await_bytes(out_ref.at[:, pl.ds(0, (nb - 2) * columns)], f_came)

        @pl.when(jnp.logical_not(is_end))
        def _():
            await_bytes(out_ref.at[:, pl.ds(0, (nb - 1) * columns)], f_came)

    with jax.named_scope("drain"):
        w_swap.wait_send()
        await_bytes(stage.at[pl.ds(0, m - 1)], a_sent)
        await_bytes(far, k_sent)
        await_bytes(att.at[:, pl.ds(0, side)], b_sent)

        @pl.when(is_gate)
        def _():
            await_bytes(att.at[:, pl.ds(0, side * (side - 1))], passed)

        @pl.when(is_end)
        def _():
            await_bytes(part_send.at[0], d_sent)
            await_bytes(part_send.at[pl.ds(0, nb - 1), pl.ds(0, nx - 1)], r_sent)
            if nb > 2:
                await_bytes(final_send.at[pl.ds(0, nb - 2)], f_sent)

        @pl.when(jnp.logical_not(is_end))
        def _():
            await_bytes(part_send.at[:, pl.ds(0, nx - 1)], r_sent)
            await_bytes(final_send.at[pl.ds(0, nb - 1)], f_sent)


def fused(nb, nu, query, keys, values, out_weight, out_gain):
    nx = nu // 2
    m = nb * nx
    rows, width = query.shape
    pairs = width // LANES // m
    depth, columns = out_weight.shape
    bf16, f32 = jnp.bfloat16, jnp.float32
    vmem, dma = pltpu.VMEM, pltpu.SemaphoreType.DMA
    in_hbm = pl.BlockSpec(memory_space=pltpu.HBM)
    block = nx * rows
    gathered = pl.pallas_call(
        functools.partial(attend_kernel, nb, nu),
        out_shape=vmem((rows, nb * columns), bf16),
        in_specs=[in_hbm] * 5,
        out_specs=pl.BlockSpec(memory_space=pltpu.VMEM),
        scratch_shapes=[
            vmem((3, rows, width), bf16),
            vmem((nb, 1, columns), f32),
            vmem((m, pairs, 3, rows, LANES), bf16),
            vmem((pairs, 3, m, rows, LANES), bf16),
            vmem((pairs, 2, m, rows, LANES), bf16),
            vmem((2 * depth, columns), bf16),
            vmem((pairs, nb, nb, block, LANES), bf16),
            vmem((nb, block, columns), f32),
            vmem((nb, nx, rows, columns), f32),
            vmem((nb, nx, rows, columns), bf16),
            vmem((nb, nx, rows, columns), bf16),
            vmem((nb, rows, columns), bf16),
            vmem((nx, rows, columns), bf16),
            dma, dma, dma, dma, dma, dma((pairs,)), dma, dma((pairs,)),
            pltpu.SemaphoreType.REGULAR((nb - 1,)),
            dma, dma((max(pairs - 1, 1), nb - 1)), dma((nb - 1, nb)), dma, dma, dma((nb, nx - 1)), dma, dma, dma, dma,
        ],
        compiler_params=pltpu.CompilerParams(
            collective_id=0, has_side_effects=True),
    )(query, keys, values, out_weight, out_gain.reshape(nb, 1, columns))
    return gathered


def on_any(nb, nu, query, keys, values, out_weight, out_gain):
    rows, width = query.shape
    suits = (
        nu % 2 == 0 and nu > 2 and nb % 2 == 0 and width % (LANES * nb * nu // 2) == 0
        and rows % 8 == 0 and (nu // 2 * rows) % 16 == 0 and (width // nb) % LANES == 0
    )
    plan = functools.partial(fused, nb, nu) if suits else on_device
    return plan(query, keys, values, out_weight, out_gain)


def solution(mesh):
    in_specs = (
        P(("group", "blk", "uly"), None),
        P(("group", "blk", "uly"), None),
        P(("group", "blk", "uly"), None),
        P("uly", "blk"),
        P(),
    )
    out_specs = P(("group", "blk", "uly"), None)
    body = functools.partial(on_any, mesh.shape["blk"], mesh.shape["uly"])
    return jax.shard_map(
        body, mesh=mesh, in_specs=in_specs, out_specs=out_specs, check_vma=False
    )
```
